256 devices in a mesh: dom: 64 (over x, z, core), rep: 4 (over y).
Axes of the slice: x: 4, y: 4, z: 8, core: 2. Of those that a mesh axis runs over, the one named last changes fastest.
Arguments:
- features: bfloat16 [524288, 128], P('dom'), may hold values from -6 to 6
- partition_map: int32 [524288], replicated, may hold values from 0 to 524287, as said below
- seed_ids: int32 [16384], P(('dom', 'rep')), may hold values from 0 to 524287, as said below
- hop1_ids: int32 [16384, 15], P(('dom', 'rep')), may hold values from 0 to 524287, as said below
- hop2_ids: int32 [16384, 15, 10], P(('dom', 'rep')), may hold values from 0 to 524287, as said below
- labels: int32 [16384], P(('dom', 'rep')), may hold values from 0 to 171
- self_one: bfloat16 [128, 256], replicated, may hold values from -0.5 to 0.5
- neigh_one: bfloat16 [128, 256], replicated, may hold values from -0.5 to 0.5
- bias_one: float32 [256], replicated, may hold values from -3 to 3
- self_two: bfloat16 [256, 172], replicated, may hold values from -0.375 to 0.375
- neigh_two: bfloat16 [256, 172], replicated, may hold values from -0.375 to 0.375
- bias_two: float32 [172], replicated, may hold values from -2 to 112, as said below
Outputs:
- seed_loss: float32 [16384], P(('dom', 'rep'))
- grad_self_one: float32 [128, 256], replicated
- grad_neigh_one: float32 [128, 256], replicated
- grad_bias_one: float32 [256], replicated
- grad_self_two: float32 [256, 172], replicated
- grad_neigh_two: float32 [256, 172], replicated
- grad_bias_two: float32 [172], replicated
The draws below stay inside these ranges and needn't reach their ends.
Inputs may be any that keep to these rules, and one draw needn't show every extreme that they name: A permutation of 0 to 524287: node v is stored at position p = partition_map[v], in partition p // 8192, row p % 8192. Rows below 256 of each partition hold hub nodes. `seed_ids`: node ids. `hop1_ids`: node ids. `hop2_ids`: take one device's 64 seeds (an aligned block of seeds) with all their hop-1 and hop-2 ids, 10624 ids with repeats counted, and map them through partition_map: at most 607 positions fall in any one partition, and at most 83 fall in rows 256 and above of any one partition. Every device reaches both bounds. `bias_two`: class biases; in one draw all 172 lie within a window of width 4 (about -2 to 2, or about 108 to 112).
All inputs are finite; a program needn't handle non-finite values.
Results may differ from the reference program's by a relative error of at most 0.003.
Values may be sent and summed in bfloat16 or wider, within the bound.
A program may use at most 128 MiB of HBM per device.

```python
import jax
import jax.numpy as jnp
from jax import lax

FEAT = 128
HID = 256
CLASSES = 172
FAN1 = 15
FAN2 = 10
HOT_DEV = 256
SEEDS_DEV = 64
NODE_DEV = 8192
TREE = 166
COLD_CAP = 83
LOW_HOT = 20
HIGH_HOT = 524
HUBS = 8
NODES = 524288
SEEDS_ALL = 16384
N_DOM = 64
N_REP = 4


def sample_plan(key):
    folded = jax.random.fold_in(key, 4242)
    key_map, key_hub, key_dev = jax.random.split(folded, 3)
    part_map = jax.random.permutation(key_map, NODES).astype(jnp.int32)
    hub_order = jax.random.permutation(key_hub, N_DOM).astype(jnp.int32)
    total_rows = SEEDS_DEV * TREE
    cold_total = N_DOM * COLD_CAP
    hub_total = HUBS * HIGH_HOT

    def one_device(dev_key):
        key_cold, key_hot, key_mix = jax.random.split(dev_key, 3)
        row_index = jnp.arange(total_rows, dtype=jnp.int32)
        is_cold = row_index < cold_total
        cold_owner = jnp.minimum(row_index // COLD_CAP, N_DOM - 1)
        hot_index = jnp.maximum(row_index - cold_total, 0)
        owner_rank = jnp.where(hot_index < hub_total, hot_index // HIGH_HOT, HUBS + (hot_index - hub_total) // LOW_HOT)
        hot_owner = hub_order[jnp.clip(owner_rank, 0, N_DOM - 1)]
        owners = jnp.where(is_cold, cold_owner, hot_owner)
        cold_row = jax.random.randint(key_cold, (total_rows,), HOT_DEV, NODE_DEV, dtype=jnp.int32)
        hot_row = jax.random.randint(key_hot, (total_rows,), 0, HOT_DEV, dtype=jnp.int32)
        store_place = owners * NODE_DEV + jnp.where(is_cold, cold_row, hot_row)
        return store_place[jax.random.permutation(key_mix, total_rows)]
    places = jax.vmap(one_device)(jax.random.split(key_dev, N_DOM * N_REP))
    inverse = jnp.zeros((NODES,), jnp.int32).at[part_map].set(jnp.arange(NODES, dtype=jnp.int32))
    return (part_map, inverse[places])


def draw_partition_map(key, part):
    part_map, node_ids = sample_plan(key)
    return part_map


def draw_seed_ids(key, part):
    part_map, node_ids = sample_plan(key)
    return node_ids[:, :SEEDS_DEV].reshape(-1)


def draw_hop1_ids(key, part):
    part_map, node_ids = sample_plan(key)
    return node_ids[:, SEEDS_DEV:SEEDS_DEV * (1 + FAN1)].reshape(N_DOM * N_REP * SEEDS_DEV, FAN1)


def draw_hop2_ids(key, part):
    part_map, node_ids = sample_plan(key)
    return node_ids[:, SEEDS_DEV * (1 + FAN1):].reshape(N_DOM * N_REP * SEEDS_DEV, FAN1, FAN2)


def draw_bias_two(key, part):
    centred = 0.5 * jax.random.truncated_normal(key, -4.0, 4.0, (CLASSES,), jnp.float32)
    return centred


def set_ends(result, key, low, high):
    shape = result.shape
    index_at = [jax.random.randint(jax.random.fold_in(key, axis), (), 0, shape[axis]) for axis in range(len(shape))]
    result = result.at[tuple(index_at)].set(low)
    longest = shape.index(max(shape))
    index_at[longest] = (index_at[longest] + 1) % shape[longest]
    return result.at[tuple(index_at)].set(high)


def shard_levels(stream_key, dims, cuts, smallest, largest):
    loudness = 1.0
    for axis_at, parts in cuts:
        heights = jax.random.uniform(jax.random.fold_in(jax.random.fold_in(stream_key, 6), axis_at), (parts,), jnp.float32, smallest / len(cuts), largest / len(cuts))
        loudness = loudness * jnp.repeat(jnp.exp(heights), dims[axis_at] // parts).reshape((-1,) + (1,) * (len(dims) - 1 - axis_at))
    return loudness


def noise(stream_key, dims, scale, reach, cuts=(), kind=jnp.bfloat16):
    drawn = scale * jax.random.normal(stream_key, dims, jnp.float32)
    if cuts:
        drawn = drawn * shard_levels(stream_key, dims, cuts, -0.22, 0.18)
    return jnp.clip(drawn, -reach, reach).astype(kind)


def setup_inputs(seed: int = 0) -> dict:
    key_list = jax.random.split(jax.random.key(seed), 13)
    features = noise(key_list[0], (NODES, FEAT), 1.0, 6.0, ((0, 64),))
    partition_map = draw_partition_map(jax.random.fold_in(key_list[12], 71), 0)
    seed_ids = draw_seed_ids(jax.random.fold_in(key_list[12], 71), 0)
    hop1_ids = draw_hop1_ids(jax.random.fold_in(key_list[12], 71), 0)
    hop2_ids = draw_hop2_ids(jax.random.fold_in(key_list[12], 71), 0)
    labels = set_ends(jax.random.randint(key_list[5], (SEEDS_ALL,), 0, CLASSES), jax.random.fold_in(key_list[5], 1), 0, CLASSES - 1).astype(jnp.int32)
    self_one = noise(key_list[6], (FEAT, HID), FEAT ** -0.5, 0.5)
    neigh_one = noise(key_list[7], (FEAT, HID), FEAT ** -0.5, 0.5)
    bias_one = noise(key_list[8], (HID,), 0.5, 3.0, (), jnp.float32)
    self_two = noise(key_list[9], (HID, CLASSES), HID ** -0.5, 0.375)
    neigh_two = noise(key_list[10], (HID, CLASSES), HID ** -0.5, 0.375)
    bias_two = draw_bias_two(jax.random.fold_in(key_list[12], 71), 0)
    return {"features": features, "partition_map": partition_map, "seed_ids": seed_ids, "hop1_ids": hop1_ids, "hop2_ids": hop2_ids, "labels": labels, "self_one": self_one, "neigh_one": neigh_one, "bias_one": bias_one, "self_two": self_two, "neigh_two": neigh_two, "bias_two": bias_two}


def activate(values):
    return jax.nn.gelu(values, approximate=True)

def sage_terms(seed_rows, hop_rows, far_rows, labels, self_one, neigh_one, bias_one, self_two, neigh_two, bias_two):
    seed_count = seed_rows.shape[0]
    fan_one = hop_rows.shape[0] // seed_count
    feat_width = seed_rows.shape[1]
    hidden = self_one.shape[1]
    seed_mean = lax.optimization_barrier(jnp.mean(hop_rows.reshape(seed_count, fan_one, feat_width), axis=1, dtype=jnp.float32)).astype(jnp.bfloat16)
    far_mean = lax.optimization_barrier(jnp.mean(far_rows, axis=1, dtype=jnp.float32)).astype(jnp.bfloat16)
    pre_seed = jnp.dot(seed_rows, self_one, preferred_element_type=jnp.float32) + jnp.dot(seed_mean, neigh_one, preferred_element_type=jnp.float32) + bias_one
    pre_hop = jnp.dot(hop_rows, self_one, preferred_element_type=jnp.float32) + jnp.dot(far_mean, neigh_one, preferred_element_type=jnp.float32) + bias_one
    act_seed, back_seed = jax.vjp(activate, pre_seed)
    act_hop, back_hop = jax.vjp(activate, pre_hop)
    hid_seed = act_seed.astype(jnp.bfloat16)
    hid_hop = act_hop.astype(jnp.bfloat16)
    hop_mean = lax.optimization_barrier(jnp.mean(hid_hop.reshape(seed_count, fan_one, hidden), axis=1, dtype=jnp.float32)).astype(jnp.bfloat16)
    logits = jnp.dot(hid_seed, self_two, preferred_element_type=jnp.float32) + jnp.dot(hop_mean, neigh_two, preferred_element_type=jnp.float32) + bias_two
    peak_value = lax.optimization_barrier(jnp.max(logits, axis=1, keepdims=True))
    shifted = logits - peak_value
    log_total = jnp.log(lax.optimization_barrier(jnp.sum(jnp.exp(shifted), axis=1, keepdims=True)))
    log_probs = shifted - log_total
    class_iota = lax.broadcasted_iota(jnp.int32, logits.shape, 1)
    target = (labels[:, None] == class_iota).astype(jnp.float32)
    seed_loss = -lax.optimization_barrier(jnp.sum(log_probs * target, axis=1))
    d_logits = ((jnp.exp(log_probs) - target) / seed_count).astype(jnp.bfloat16)
    grad_self_two = jnp.dot(hid_seed.T, d_logits, preferred_element_type=jnp.float32)
    grad_neigh_two = jnp.dot(hop_mean.T, d_logits, preferred_element_type=jnp.float32)
    grad_bias_two = lax.optimization_barrier(jnp.sum(d_logits.astype(jnp.float32), axis=0))
    d_hid_seed = jnp.dot(d_logits, self_two.T, preferred_element_type=jnp.float32)
    d_hop_mean = jnp.dot(d_logits, neigh_two.T, preferred_element_type=jnp.float32)
    d_pre_seed = back_seed(d_hid_seed)[0].astype(jnp.bfloat16)
    spread = jnp.broadcast_to((d_hop_mean / fan_one)[:, None, :], (seed_count, fan_one, hidden)).reshape(seed_count * fan_one, hidden)
    d_pre_hop = back_hop(spread)[0].astype(jnp.bfloat16)
    grad_self_one = jnp.dot(seed_rows.T, d_pre_seed, preferred_element_type=jnp.float32) + jnp.dot(hop_rows.T, d_pre_hop, preferred_element_type=jnp.float32)
    grad_neigh_one = jnp.dot(seed_mean.T, d_pre_seed, preferred_element_type=jnp.float32) + jnp.dot(far_mean.T, d_pre_hop, preferred_element_type=jnp.float32)
    grad_bias_one = lax.optimization_barrier(jnp.sum(d_pre_seed.astype(jnp.float32), axis=0)) + lax.optimization_barrier(jnp.sum(d_pre_hop.astype(jnp.float32), axis=0))
    return (seed_loss, (grad_self_one, grad_neigh_one, grad_bias_one, grad_self_two, grad_neigh_two, grad_bias_two))

def reference(features, partition_map, seed_ids, hop1_ids, hop2_ids, labels, self_one, neigh_one, bias_one, self_two, neigh_two, bias_two):
    devices = N_DOM * N_REP
    seed_blocks = seed_ids.reshape(devices, SEEDS_DEV)
    hop_blocks = hop1_ids.reshape(devices, SEEDS_DEV * FAN1)
    far_blocks = hop2_ids.reshape(devices, SEEDS_DEV * FAN1, FAN2)
    label_blocks = labels.reshape(devices, SEEDS_DEV)
    initial = (jnp.zeros((FEAT, HID), jnp.float32), jnp.zeros((FEAT, HID), jnp.float32), jnp.zeros((HID,), jnp.float32), jnp.zeros((HID, CLASSES), jnp.float32), jnp.zeros((HID, CLASSES), jnp.float32), jnp.zeros((CLASSES,), jnp.float32))

    def one_block(totals, pieces):
        seeds_here, hops_here, far_here, labels_here = pieces
        seed_rows = features[partition_map[seeds_here]]
        hop_rows = features[partition_map[hops_here]]
        far_rows = features[partition_map[far_here]]
        seed_loss, grads = sage_terms(seed_rows, hop_rows, far_rows, labels_here, self_one, neigh_one, bias_one, self_two, neigh_two, bias_two)
        return (jax.tree.map(jnp.add, totals, grads), seed_loss)
    totals, losses = lax.scan(one_block, initial, (seed_blocks, hop_blocks, far_blocks, label_blocks))
    return (losses.reshape(-1), totals[0], totals[1], totals[2], totals[3], totals[4], totals[5])
```

```python
import functools

import jax
import jax.numpy as jnp
from jax import lax
from jax.experimental import pallas as pl
from jax.experimental.pallas import tpu as pltpu
from jax.sharding import PartitionSpec as P

HOT_DEV = 256
LANES = 128
MESH = pl.DeviceIdType.MESH
VMEM_LIMIT = 56 * 1024 * 1024


def round_up(value, unit):
    return -(-value // unit) * unit


def dot_tn(left, right):
    return lax.dot_general(left, right, (((0,), (0,)), ((), ())), preferred_element_type=jnp.float32)


def dot_nt(left, right):
    return lax.dot_general(left, right, (((1,), (1,)), ((), ())), preferred_element_type=jnp.float32)


def dot_nn(left, right):
    return jnp.dot(left, right, preferred_element_type=jnp.float32)


N_X, N_Z = 4, 8
ID_ROWS = 83
HUB_ROWS = 64 * HOT_DEV


def place_ids(hop2_ref, hop1_ref, seed_ref, ids_ref):
    fan_two, fan_one, seeds = hop2_ref.shape
    half = fan_two // 2
    ids_ref[...] = jnp.zeros(ids_ref.shape, jnp.int32)
    for m in range(half):
        at = slice(m * fan_one, (m + 1) * fan_one)
        ids_ref[at, :seeds] = hop2_ref[m]
        ids_ref[at, seeds:] = hop2_ref[half + m]
    top = half * fan_one
    ids_ref[top : top + 8, :seeds] = hop1_ref[:8, :]
    ids_ref[top : top + fan_one - 8, seeds:] = hop1_ref[8:, :]
    ids_ref[top + fan_one - 8 : top + fan_one - 7, seeds:] = seed_ref[...]


def gather_map(first, smem_ref, map_ref, stage):
    for r in range(stage.shape[0] // LANES):
        for i in range(LANES):
            stage[pl.ds(r * LANES + i, 1), :] = map_ref[pl.ds(smem_ref[first + r, i] >> 7, 1), :]


def pick_lanes(first, ids_ref, stage, pos_ref):
    sub_iota = lax.broadcasted_iota(jnp.int32, (LANES, LANES), 0)
    lane_iota = lax.broadcasted_iota(jnp.int32, (LANES, LANES), 1)
    for r in range(stage.shape[0] // LANES):
        got = stage[r * LANES : (r + 1) * LANES, :]
        pieces = jnp.concatenate([got >> 16, (got >> 8) & 255, got & 255], axis=0)
        pieces = pieces.astype(jnp.float32).astype(jnp.bfloat16)
        low = ids_ref[pl.ds(first + r, 1), :] & (LANES - 1)
        hot = (sub_iota == low).astype(jnp.float32).astype(jnp.bfloat16)
        found = dot_nn(pieces, hot)
        found = found[:LANES] * 65536.0 + found[LANES : 2 * LANES] * 256.0 + found[2 * LANES :]
        picked = jnp.sum(jnp.where(sub_iota == lane_iota, found, 0.0), axis=0, keepdims=True)
        pos_ref[pl.ds(first + r, 1), :] = picked.astype(jnp.int32)


def lookup_step(step, ids_ref, smem_ref, map_ref, stage_a, stage_b, pos_ref):
    first = step * 4
    gather_map(first, smem_ref, map_ref, stage_a)

    pick_lanes(first, ids_ref, stage_a, pos_ref)
    gather_map(first + 2, smem_ref, map_ref, stage_b)
    pick_lanes(first + 2, ids_ref, stage_b, pos_ref)


def assign(pos_ref, own_ref, val_ref, slot_ref, addr_ref, req_ref, *, parts, shift, cap_row):
    rows = pos_ref.shape[0]
    position = pos_ref[...]
    owner = position >> shift
    local = position & ((1 << shift) - 1)
    row_iota = lax.broadcasted_iota(jnp.int32, (rows, LANES), 0)
    is_cold = (local >= HOT_DEV) & (row_iota < ID_ROWS)
    own_ref[...] = jnp.where(is_cold, owner, -1)
    val_ref[...] = local
    part_iota = lax.broadcasted_iota(jnp.int32, (parts, LANES), 0)
    slot_iota = lax.broadcasted_iota(jnp.int32, (LANES, LANES), 0)
    upper = lax.broadcasted_iota(jnp.int32, (LANES, 2 * LANES), 0) <= lax.broadcasted_iota(
        jnp.int32, (LANES, 2 * LANES), 1
    )
    upper = upper.astype(jnp.float32).astype(jnp.bfloat16)

    def block(step, carry):
        base, table = carry
        at = pl.ds(pl.multiple_of(step * 8, 8), 8)
        own8 = own_ref[at, :]
        val8 = val_ref[at, :].astype(jnp.float32)
        top8 = jnp.floor(val8 * (1.0 / LANES))
        low8 = val8 - top8 * LANES
        slots, lefts = [], []
        for q in range(8):
            mine = part_iota == own8[q : q + 1, :]
            counts = dot_nn(mine.astype(jnp.float32).astype(jnp.bfloat16), upper)
            slots.append(jnp.sum(jnp.where(mine, counts[:, :LANES] + base, 0.0), axis=0, keepdims=True) - 1.0)
            base = base + counts[:, LANES:]
            lefts.append(
                jnp.concatenate(
                    [jnp.where(mine, top8[q : q + 1, :], 0.0), jnp.where(mine, low8[q : q + 1, :], 0.0)], axis=0
                ).astype(jnp.bfloat16)
            )
        slot8 = jnp.concatenate(slots, axis=0).astype(jnp.int32)
        slot_ref[at, :] = slot8
        for q in range(0, 8, 2):
            rights = [
                (slot_iota == slot8[k : k + 1, :]).astype(jnp.float32).astype(jnp.bfloat16) for k in (q, q + 1)
            ]
            table = table + dot_nt(
                jnp.concatenate([lefts[q], lefts[q + 1]], axis=1), jnp.concatenate(rights, axis=1)
            )
        return base, table

    start = (jnp.zeros((parts, LANES), jnp.float32), jnp.zeros((2 * parts, LANES), jnp.float32))
    table = lax.fori_loop(0, rows // 8, block, start)[1]
    request = (table[:parts] * LANES + table[parts:]).astype(jnp.int32) & ((1 << shift) - 1)
    for p in range(parts):
        req_ref[p, 0:1, :] = request[p : p + 1, :]
    hot_addr = (owner & 1) * (HUB_ROWS // 2) + (owner >> 1) * HOT_DEV + (local & (HOT_DEV - 1))
    addr_ref[...] = jnp.where(is_cold, HUB_ROWS + owner * cap_row + slot_ref[...], hot_addr)


def front_kernel(
    hop2_ref, hop1_ref, seed_ref, map_hbm, feat_hbm,
    table_ref, addr_ref,
    ids_ref, pos_ref, own_ref, val_ref, slot_ref, map_ref, feat_ref, wide, stage_a, stage_b, row_stage,
    req_ref, inbox, send, ids_smem, wanted,
    local_sem, req_send, req_recv, hub_send, hub_recv, row_send, row_recv, *, parts, shift, cap_row,
):
    node_rows = feat_ref.shape[0]
    me = lax.axis_index("dom")
    core, z, x = lax.rem(me, 2), lax.rem(me // 2, N_Z), me // (2 * N_Z)
    barrier = pltpu.get_barrier_semaphore()

    get_map = pltpu.make_async_copy(map_hbm, map_ref, local_sem.at[0])
    get_map.start()
    get_feat = pltpu.make_async_copy(feat_hbm, feat_ref, local_sem.at[1])
    get_feat.start()
    x_rows = N_Z * HOT_DEV
    half = N_X * x_rows
    own_at = pl.ds(pl.multiple_of(core * half + (x * N_Z + z) * HOT_DEV, HOT_DEV), HOT_DEV)
    keep_hub = pltpu.make_async_copy(feat_hbm.at[pl.ds(0, HOT_DEV)], table_ref.at[own_at], local_sem.at[2])
    keep_hub.start()

    def peer(step):
        k = lax.rem(step, 8)
        dz = lax.rem(N_Z + 4 + (lax.rem(k, 2) * 2 - 1) * ((k + 1) // 2), N_Z)
        dxc = lax.rem(step // 8 + 1, 8)
        other = (lax.rem(x + dxc // 2, N_X) * N_Z + lax.rem(z + dz, N_Z)) * 2 + lax.rem(core + lax.rem(dxc, 2), 2)
        return other, {"dom": other}

    def greet(step, carry):
        pl.semaphore_signal(barrier, inc=1, device_id=peer(step)[1], device_id_type=MESH)
        return carry

    lax.fori_loop(0, parts - 1, greet, 0)

    place_ids(hop2_ref, hop1_ref, seed_ref, ids_ref)
    ids_down = pltpu.make_async_copy(ids_ref, ids_smem, local_sem.at[3])
    ids_down.start()
    get_feat.wait()

    def widen(step, carry):
        at = pl.ds(pl.multiple_of(step * 64, 64), 64)
        wide[at, :] = feat_ref[at, :].astype(jnp.float32)
        return carry

    lax.fori_loop(0, node_rows // 64, widen, 0)
    keep_hub.wait()
    pl.semaphore_wait(barrier, parts - 1)

    def hub_copy(at, level, where):
        return pltpu.make_async_remote_copy(
            table_ref.at[at], table_ref.at[at], hub_send.at[level], hub_recv.at[level],
            device_id=where, device_id_type=MESH,
        )

    def hub_wait(rows, level):
        return hub_copy(pl.ds(0, rows), level, peer(0)[1])

    def send_z(step, carry):
        hub_copy(own_at, 0, {"dom": (x * N_Z + lax.rem(z + step, N_Z)) * 2 + core}).start()
        return carry

    def x_at(step):
        return pl.ds(pl.multiple_of(core * half + lax.rem(x + step, N_X) * x_rows, x_rows), x_rows)

    def send_x(step, carry):
        hub_copy(x_at(0), 1, {"dom": (lax.rem(x + step, N_X) * N_Z + z) * 2 + core}).start()
        return carry

    def send_core(step, carry):
        hub_copy(x_at(step), 2, {"dom": me + 1 - 2 * core}).start()
        return carry

    lax.fori_loop(1, N_Z, send_z, 0)
    get_map.wait()
    ids_down.wait()

    def lookup(step, carry):
        lookup_step(step, ids_ref, ids_smem, map_ref, stage_a, stage_b, pos_ref)
        return carry

    groups = -(-ID_ROWS // 4)
    lax.fori_loop(0, groups // 3, lookup, 0)
    hub_wait((N_Z - 1) * HOT_DEV, 0).wait_recv()
    lax.fori_loop(1, N_X, send_x, 0)
    lax.fori_loop(0, 1, send_core, 0)
    lax.fori_loop(groups // 3, groups, lookup, 0)
    for r in range(groups * 4, pos_ref.shape[0]):
        pos_ref[r : r + 1, :] = jnp.zeros((1, LANES), jnp.int32)
    assign(
        pos_ref, own_ref, val_ref, slot_ref, addr_ref, req_ref, parts=parts, shift=shift, cap_row=cap_row,
    )
    ask_at = pl.ds(0, 1)
    keep_req = pltpu.make_async_copy(req_ref.at[me], inbox.at[me], local_sem.at[4])
    keep_req.start()

    def ask(step, carry):
        other, where = peer(step)
        pltpu.make_async_remote_copy(
            req_ref.at[other, ask_at], inbox.at[me, ask_at], req_send, req_recv, device_id=where, device_id_type=MESH
        ).start()
        return carry

    lax.fori_loop(0, parts - 1, ask, 0)
    most = pl.ds(0, parts - 1)
    asked = pltpu.make_async_remote_copy(
        req_ref.at[most, ask_at], inbox.at[most, ask_at], req_send, req_recv,
        device_id=peer(0)[1], device_id_type=MESH,
    )
    keep_req.wait()
    asked.wait_recv()
    to_scalar = pltpu.make_async_copy(inbox.at[:, ask_at], wanted, local_sem.at[5])
    to_scalar.start()
    to_scalar.wait()

    def collect(other):
        for i in range(cap_row):
            row_stage[i : i + 1, :] = wide[pl.ds(wanted[other, 0, i], 1), :]
        return row_stage[...].astype(jnp.bfloat16)

    def rows_at(part):
        return pl.ds(pl.multiple_of(HUB_ROWS + part * cap_row, 8), cap_row)

    def serve(step, carry):
        other, where = peer(step)
        send[other] = collect(other)
        pltpu.make_async_remote_copy(
            send.at[other], table_ref.at[rows_at(me)], row_send, row_recv, device_id=where, device_id_type=MESH
        ).start()
        return carry

    lax.fori_loop(0, parts - 1, serve, 0)
    table_ref[rows_at(me), :] = collect(me)
    hub_wait((N_X - 1) * x_rows, 1).wait_recv()
    lax.fori_loop(1, N_X, send_core, 0)
    asked.wait_send()
    hub_wait((N_Z - 1) * HOT_DEV, 0).wait_send()
    hub_wait((N_X - 1) * x_rows, 1).wait_send()
    hub_wait(half, 2).wait()
    pltpu.make_async_remote_copy(
        send.at[most], send.at[most], row_send, row_recv, device_id=peer(0)[1], device_id_type=MESH
    ).wait()


def front(hop2, hop1, seed_ids, partition_map, features, cap_row):
    parts = lax.axis_size("dom")
    node_rows, feat = features.shape
    vmem = pl.BlockSpec(memory_space=pltpu.VMEM)
    hbm = pl.BlockSpec(memory_space=pl.ANY)
    rows = round_up(ID_ROWS, 8)
    return pl.pallas_call(
        functools.partial(front_kernel, parts=parts, shift=node_rows.bit_length() - 1, cap_row=cap_row),
        name="front",
        out_shape=(
            jax.ShapeDtypeStruct((HUB_ROWS + parts * cap_row, feat), features.dtype),
            jax.ShapeDtypeStruct((rows, LANES), jnp.int32),
        ),
        in_specs=[vmem, vmem, vmem, hbm, hbm],
        out_specs=(vmem, vmem),
        scratch_shapes=[pltpu.VMEM((rows, LANES), jnp.int32)] * 5
        + [
            pltpu.VMEM((partition_map.size // LANES, LANES), jnp.int32),
            pltpu.VMEM((node_rows, feat), features.dtype),
            pltpu.VMEM((node_rows, feat), jnp.float32),
            pltpu.VMEM((2 * LANES, LANES), jnp.int32),
            pltpu.VMEM((2 * LANES, LANES), jnp.int32),
            pltpu.VMEM((cap_row, feat), jnp.float32),
            pltpu.VMEM((parts, 8, LANES), jnp.int32),
            pltpu.VMEM((parts, 8, LANES), jnp.int32),
            pltpu.VMEM((parts, cap_row, feat), features.dtype),
            pltpu.SMEM((rows, LANES), jnp.int32),
            pltpu.SMEM((parts, 1, LANES), jnp.int32),
            pltpu.SemaphoreType.DMA((6,)),
            pltpu.SemaphoreType.DMA,
            pltpu.SemaphoreType.DMA,
            pltpu.SemaphoreType.DMA((3,)),
            pltpu.SemaphoreType.DMA((3,)),
            pltpu.SemaphoreType.DMA,
            pltpu.SemaphoreType.DMA,
        ],
        compiler_params=pltpu.CompilerParams(collective_id=2, has_side_effects=True, vmem_limit_bytes=VMEM_LIMIT),
    )(hop2, hop1, seed_ids.reshape(1, -1), partition_map.reshape(-1, LANES), features)


ROOT = 0.7978845608028654
CUBE = 0.044715


def gelu_pair(pre):
    square = pre * pre
    bend = jnp.tanh(ROOT * pre * (1.0 + CUBE * square))
    half = 0.5 * (1.0 + bend)
    slope = half + 0.5 * pre * (1.0 - bend * bend) * (ROOT * (1.0 + 3.0 * CUBE * square))
    return pre * half, slope


def tree_sum(values):
    while len(values) > 1:
        values = [a + b for a, b in zip(values[::2], values[1::2])] + (
            [values[-1]] if len(values) % 2 else []
        )
    return values[0]


def model_kernel(
    addr_ref, table_ref, label_ref, self_one, neigh_one, b_one_ref, self_two, neigh_two, b_two_ref,
    loss_ref, pack_ref,
    wide, x_buf, far_buf, own_buf, slope_buf, d_buf, *, seeds, fan_one, fan_two,
):
    feat = table_ref.shape[1]
    hidden = self_one.shape[1]
    hops = seeds * fan_one
    chunk = 64 if table_ref.shape[0] % 64 == 0 else 16

    def widen(step, carry):
        at = pl.ds(pl.multiple_of(step * chunk, chunk), chunk)
        wide[at, :] = table_ref[at, :].astype(jnp.float32)
        return carry

    lax.fori_loop(0, table_ref.shape[0] // chunk, widen, 0)

    half = fan_two // 2
    top = half * fan_one

    def fetch(step, carry):
        j = step // (seeds // 8)
        block = step % (seeds // 8)
        base = pl.multiple_of(step * 8, 8)
        seed = block * 8
        own_row = jnp.where(j < 8, (top + j) * LANES, (top + j - 8) * LANES + seeds) + seed
        for k in range(8):
            own_buf[pl.ds(base + k, 1), :] = wide[pl.ds(addr_ref[own_row + k], 1), :]
            rows = [
                wide[pl.ds(addr_ref[(m % half * fan_one + j) * LANES + m // half * seeds + seed + k], 1), :]
                for m in range(fan_two)
            ]
            far_buf[pl.ds(base + k, 1), :] = tree_sum(rows)
        return carry

    lax.fori_loop(0, hops // 8, fetch, 0)

    def fetch_seed(step, carry):
        base = pl.multiple_of(step * 8, 8)
        first = (top + fan_one - 8) * LANES + seeds
        for k in range(8):
            own_buf[pl.ds(hops + base + k, 1), :] = wide[pl.ds(addr_ref[first + base + k], 1), :]
        return carry

    lax.fori_loop(0, seeds // 8, fetch_seed, 0)

    w_one = jnp.concatenate([self_one[...], neigh_one[...]], axis=0)
    w_two = jnp.concatenate([self_two[...], neigh_two[...]], axis=1)
    b_one = b_one_ref[...]
    row_sum = jnp.zeros((seeds, feat), jnp.float32)
    hid_sum = jnp.zeros((seeds, hidden), jnp.float32)
    for j in range(fan_one):
        at = slice(j * seeds, (j + 1) * seeds)
        own = own_buf[at, :]
        row_sum = row_sum + own
        x_buf[at, :feat] = own.astype(jnp.bfloat16)
        x_buf[at, feat:] = (far_buf[at, :] * (1.0 / fan_two)).astype(jnp.bfloat16)
    x_buf[hops:, :feat] = own_buf[hops:, :].astype(jnp.bfloat16)
    x_buf[hops:, feat:] = (row_sum * (1.0 / fan_one)).astype(jnp.bfloat16)
    act = None
    for j in range(fan_one + 1):
        at = slice(j * seeds, (j + 1) * seeds)
        act, slope = gelu_pair(dot_nn(x_buf[at, :], w_one) + b_one)
        act = act.astype(jnp.bfloat16)
        slope_buf[at, :] = slope
        if j < fan_one:
            hid_sum = hid_sum + act.astype(jnp.float32)
    hid = jnp.concatenate([act, (hid_sum * (1.0 / fan_one)).astype(jnp.bfloat16)], axis=1)
    logits = dot_nt(hid, w_two) + b_two_ref[...]
    shifted = logits - jnp.max(logits, axis=1, keepdims=True)
    log_probs = shifted - jnp.log(jnp.sum(jnp.exp(shifted), axis=1, keepdims=True))
    class_iota = lax.broadcasted_iota(jnp.int32, logits.shape, 1)
    diagonal = lax.broadcasted_iota(jnp.int32, (seeds, seeds), 0) == lax.broadcasted_iota(jnp.int32, (seeds, seeds), 1)
    label = jnp.sum(jnp.where(diagonal, label_ref[...].astype(jnp.float32), 0.0), axis=1, keepdims=True)
    target = (class_iota.astype(jnp.float32) == label).astype(jnp.float32)
    loss = jnp.sum(log_probs * target, axis=1, keepdims=True)
    loss_ref[...] = -jnp.sum(jnp.where(diagonal, loss, 0.0), axis=0, keepdims=True)
    d_logits = ((jnp.exp(log_probs) - target) * (1.0 / seeds)).astype(jnp.bfloat16)
    g_two = dot_tn(d_logits, hid)
    gb_two = jnp.sum(d_logits.astype(jnp.float32), axis=0, keepdims=True)
    d_hid = dot_nn(d_logits, w_two)
    d_hop = d_hid[:, hidden:] * (1.0 / fan_one)
    for j in range(fan_one + 1):
        at = slice(j * seeds, (j + 1) * seeds)
        d_pre = ((d_hop if j < fan_one else d_hid[:, :hidden]) * slope_buf[at, :]).astype(jnp.bfloat16)
        d_buf[at, :] = d_pre
    gb_one = dot_nn(jnp.ones((8, d_buf.shape[0]), jnp.bfloat16), d_buf[...])[:1]
    pack_gradients(pack_ref, dot_tn(x_buf[...], d_buf[...]), gb_one, g_two, gb_two)


def model(addr, table, labels, self_one, neigh_one, bias_one, self_two, neigh_two, bias_two, fan_one, fan_two, pack_rows):
    seeds = labels.shape[0]
    feat, hidden = self_one.shape
    classes = self_two.shape[1]
    total = seeds * (1 + fan_one)
    vmem = pl.BlockSpec(memory_space=pltpu.VMEM)
    return pl.pallas_call(
        functools.partial(model_kernel, seeds=seeds, fan_one=fan_one, fan_two=fan_two),
        name="model",
        out_shape=(
            jax.ShapeDtypeStruct((1, seeds), jnp.float32),
            jax.ShapeDtypeStruct((pack_rows, LANES), jnp.float32),
        ),
        in_specs=[pl.BlockSpec(memory_space=pltpu.SMEM)] + [vmem] * 8,
        out_specs=(vmem,) * 2,
        scratch_shapes=[
            pltpu.VMEM(table.shape, jnp.float32),
            pltpu.VMEM((total, 2 * feat), jnp.bfloat16),
            pltpu.VMEM((total - seeds, feat), jnp.float32),
            pltpu.VMEM((total, feat), jnp.float32),
            pltpu.VMEM((total, hidden), jnp.float32),
            pltpu.VMEM((total, hidden), jnp.bfloat16),
        ],
        compiler_params=pltpu.CompilerParams(vmem_limit_bytes=VMEM_LIMIT),
        cost_estimate=pl.CostEstimate(flops=100_000_000, bytes_accessed=4_000_000, transcendentals=0),
    )(
        addr,
        table,
        labels.reshape(1, seeds),
        self_one,
        neigh_one,
        bias_one.reshape(1, hidden),
        self_two.T,
        neigh_two.T,
        bias_two.reshape(1, classes),
    )


def pack_plan(feat, hidden, classes):
    halves = hidden // LANES
    one = 2 * feat * halves
    high = round_up(classes, 8)
    tail = one + 2 * halves * high
    return halves, one, high, tail, tail + 8


def pack_gradients(pack_ref, g_one, gb_one, g_two, gb_two):
    hidden, feat = g_one.shape[1], g_one.shape[0] // 2
    classes = g_two.shape[0]
    halves, one, high, tail, used = pack_plan(feat, hidden, classes)
    for h in range(halves):
        pack_ref[h * 2 * feat : (h + 1) * 2 * feat, :] = g_one[:, h * LANES : (h + 1) * LANES]
    pack_ref[one:, :] = jnp.zeros((pack_ref.shape[0] - one, LANES), jnp.float32)
    for h in range(2 * halves):
        pack_ref[one + h * high : one + h * high + classes, :] = g_two[:, h * LANES : (h + 1) * LANES]
    for h in range(halves):
        pack_ref[tail + h : tail + h + 1, :] = gb_one[:, h * LANES : (h + 1) * LANES]
    pack_ref[tail + halves : tail + halves + 1, :] = gb_two[:, :LANES]
    pack_ref[tail + halves + 1 : tail + halves + 2, : classes - LANES] = gb_two[:, LANES:]


def unpack_kernel(pack_ref, self_one, neigh_one, bias_one, self_two, neigh_two, bias_two):
    feat, hidden = self_one.shape
    classes = self_two.shape[0]
    halves, one, high, tail, used = pack_plan(feat, hidden, classes)
    for h in range(halves):
        cols = slice(h * LANES, (h + 1) * LANES)
        at = h * 2 * feat
        self_one[:, cols] = pack_ref[at : at + feat, :]
        neigh_one[:, cols] = pack_ref[at + feat : at + 2 * feat, :]
        at = one + h * high
        self_two[:, cols] = pack_ref[at : at + classes, :]
        at = one + (halves + h) * high
        neigh_two[:, cols] = pack_ref[at : at + classes, :]
        bias_one[:, cols] = pack_ref[tail + h : tail + h + 1, :]
    bias_two[:, :LANES] = pack_ref[tail + halves : tail + halves + 1, :]
    bias_two[:, LANES:] = pack_ref[tail + halves + 1 : tail + halves + 2, : classes - LANES]


def unpack(packed, feat, hidden, classes):
    vmem = pl.BlockSpec(memory_space=pltpu.VMEM)
    shapes = [(feat, hidden), (feat, hidden), (1, hidden), (classes, hidden), (classes, hidden), (1, classes)]
    return pl.pallas_call(
        unpack_kernel,
        name="unpack",
        out_shape=tuple(jax.ShapeDtypeStruct(shape, jnp.float32) for shape in shapes),
        in_specs=[vmem],
        out_specs=(vmem,) * 6,
        compiler_params=pltpu.CompilerParams(vmem_limit_bytes=VMEM_LIMIT),
    )(packed)


def reduce_kernel(
    part_ref, out_ref, near_box, middle, far_box, gathered, send_sem, recv_sem, *, n_dom, n_rep, near,
):
    count = n_dom * n_rep
    far = count // near
    rows = part_ref.shape[0] // count
    span = far * rows
    me = lax.axis_index("dom") * n_rep + lax.axis_index("rep")
    here, there = lax.rem(me, near), me // near
    barrier = pltpu.get_barrier_semaphore()

    def place(index):
        return {"dom": index // n_rep, "rep": lax.rem(index, n_rep)}

    def near_peer(step):
        other = lax.rem(here + step, near)
        return other, place(there * near + other)

    def far_peer(step):
        other = lax.rem(there + step, far)
        return other, place(other * near + here)

    def wide_at(index):
        return pl.ds(pl.multiple_of(index * span, 8), span)

    def thin_at(index):
        return pl.ds(pl.multiple_of(index * rows, 8), rows)

    def greet_near(step, carry):
        pl.semaphore_signal(barrier, inc=1, device_id=near_peer(step)[1], device_id_type=MESH)
        return carry

    def greet_far(step, carry):
        pl.semaphore_signal(barrier, inc=1, device_id=far_peer(step)[1], device_id_type=MESH)
        return carry

    lax.fori_loop(1, near, greet_near, 0)
    lax.fori_loop(1, far, greet_far, 0)
    pl.semaphore_wait(barrier, near + far - 2)

    def copy(source, target, stage, where):
        return pltpu.make_async_remote_copy(
            source, target, send_sem.at[stage], recv_sem.at[stage], device_id=where, device_id_type=MESH
        )

    def out_near(step, carry):
        other, where = near_peer(step)
        copy(part_ref.at[wide_at(other)], near_box.at[wide_at(here)], 0, where).start()
        return carry

    lax.fori_loop(1, near, out_near, 0)
    some = pl.ds(0, (near - 1) * span)
    first = copy(part_ref.at[some], near_box.at[some], 0, near_peer(1)[1])
    first.wait_recv()

    def add_near(step, total):
        return total + near_box[wide_at(near_peer(step)[0]), :]

    middle[...] = lax.fori_loop(1, near, add_near, part_ref[wide_at(here), :])

    def out_far(step, carry):
        other, where = far_peer(step)
        copy(middle.at[thin_at(other)], far_box.at[thin_at(there)], 1, where).start()
        return carry

    lax.fori_loop(1, far, out_far, 0)
    some = pl.ds(0, (far - 1) * rows)
    second = copy(middle.at[some], far_box.at[some], 1, far_peer(1)[1])
    second.wait_recv()

    def add_far(step, total):
        return total + far_box[thin_at(far_peer(step)[0]), :]

    total = lax.fori_loop(1, far, add_far, middle[thin_at(there), :])
    mine = here * far + there
    gathered[mine] = total.astype(gathered.dtype)

    def back_far(step, carry):
        copy(gathered.at[mine], gathered.at[mine], 2, far_peer(step)[1]).start()
        return carry

    lax.fori_loop(1, far, back_far, 0)
    some = gathered.at[pl.ds(0, far - 1)]
    third = copy(some, some, 2, far_peer(1)[1])
    third.wait_recv()
    group = gathered.at[pl.ds(here * far, far)]

    def back_near(step, carry):
        copy(group, group, 3, near_peer(step)[1]).start()
        return carry

    lax.fori_loop(1, near, back_near, 0)
    some = gathered.at[pl.ds(0, (near - 1) * far)]
    fourth = copy(some, some, 3, near_peer(1)[1])
    fourth.wait_recv()
    first.wait_send()
    second.wait_send()
    third.wait_send()
    fourth.wait_send()
    for index in range(count):
        out_ref[index * rows : (index + 1) * rows, :] = gathered[index].astype(jnp.float32)


def sum_everywhere(pieces):
    n_dom, n_rep = lax.axis_size("dom"), lax.axis_size("rep")
    count = n_dom * n_rep
    near = 8
    far = count // near
    rows = pieces.shape[0] // count
    vmem = pl.BlockSpec(memory_space=pltpu.VMEM)
    return pl.pallas_call(
        functools.partial(reduce_kernel, n_dom=n_dom, n_rep=n_rep, near=near),
        name="sum_everywhere",
        out_shape=jax.ShapeDtypeStruct(pieces.shape, jnp.float32),
        in_specs=[vmem],
        out_specs=vmem,
        scratch_shapes=[
            pltpu.VMEM(pieces.shape, jnp.float32),
            pltpu.VMEM((far * rows, LANES), jnp.float32),
            pltpu.VMEM((far * rows, LANES), jnp.float32),
            pltpu.VMEM((count, rows, LANES), jnp.bfloat16),
            pltpu.SemaphoreType.DMA((4,)),
            pltpu.SemaphoreType.DMA((4,)),
        ],
        compiler_params=pltpu.CompilerParams(collective_id=1, has_side_effects=True, vmem_limit_bytes=VMEM_LIMIT),
    )(pieces)


def shards(
    features, partition_map, seed_ids, hop1_ids, hop2_ids, labels,
    self_one, neigh_one, bias_one, self_two, neigh_two, bias_two,
):
    parts = lax.axis_size("dom")
    count = parts * lax.axis_size("rep")
    seeds = seed_ids.shape[0]
    fan_one = hop1_ids.shape[1]
    fan_two = hop2_ids.shape[2]
    feat = features.shape[1]
    tree_rows = 1 + fan_one + fan_one * fan_two
    cold_cap = tree_rows // 2 * (seeds // parts)
    cap_row = round_up(cold_cap, 8)
    table, addr = front(hop2_ids.transpose(2, 1, 0), hop1_ids.T, seed_ids, partition_map, features, cap_row)
    hidden, classes = self_two.shape
    used = pack_plan(feat, hidden, classes)[-1]
    pack_rows = count * round_up(-(-used // count), 8)
    loss, pieces = model(
        addr.reshape(-1), table, labels, self_one, neigh_one, bias_one, self_two, neigh_two, bias_two,
        fan_one, fan_two, pack_rows,
    )
    grads = unpack(sum_everywhere(pieces), feat, hidden, classes)
    return (
        loss.reshape(-1), grads[0], grads[1], grads[2].reshape(-1),
        grads[3].T, grads[4].T, grads[5].reshape(-1),
    )


def solution(mesh):
    return jax.shard_map(
        shards,
        mesh=mesh,
        in_specs=(
            P("dom", None),
            P(),
            P(("dom", "rep")),
            P(("dom", "rep"), None),
            P(("dom", "rep"), None, None),
            P(("dom", "rep")),
            P(),
            P(),
            P(),
            P(),
            P(),
            P(),
        ),
        out_specs=(P(("dom", "rep")), P(), P(), P(), P(), P(), P()),
        check_vma=False,
    )
```

```python
import functools

import jax
import jax.numpy as jnp
from jax import lax
from jax.experimental import pallas as pl
from jax.experimental.pallas import tpu as pltpu
from jax.sharding import PartitionSpec as P

HOT_DEV = 256
LANES = 128
MESH = pl.DeviceIdType.MESH
MIB = 1024 * 1024


def round_up(value, unit):
    return -(-value // unit) * unit


def dot_tn(left, right):
    return lax.dot_general(left, right, (((0,), (0,)), ((), ())), preferred_element_type=jnp.float32)


def dot_nt(left, right):
    return lax.dot_general(left, right, (((1,), (1,)), ((), ())), preferred_element_type=jnp.float32)


def dot_nn(left, right):
    return jnp.dot(left, right, preferred_element_type=jnp.float32)


N_X, N_Z = 4, 8
ID_ROWS = 83
HUB_ROWS = 64 * HOT_DEV


def place_ids(hop2_ref, hop1_ref, seed_ref, ids_ref):
    fan_two, fan_one, seeds = hop2_ref.shape
    half = fan_two // 2
    ids_ref[...] = jnp.zeros(ids_ref.shape, jnp.int32)
    for m in range(half):
        at = slice(m * fan_one, (m + 1) * fan_one)
        ids_ref[at, :seeds] = hop2_ref[m]
        ids_ref[at, seeds:] = hop2_ref[half + m]
    top = half * fan_one
    ids_ref[top : top + 8, :seeds] = hop1_ref[:8, :]
    ids_ref[top : top + fan_one - 8, seeds:] = hop1_ref[8:, :]
    ids_ref[top + fan_one - 8 : top + fan_one - 7, seeds:] = seed_ref[...]


def gather_map(first, smem_ref, map_ref, stage):
    for r in range(stage.shape[0] // LANES):
        for i in range(LANES):
            stage[pl.ds(r * LANES + i, 1), :] = map_ref[pl.ds(smem_ref[first + r, i] >> 7, 1), :]


def pick_lanes(first, ids_ref, stage, pos_ref):
    sub_iota = lax.broadcasted_iota(jnp.int32, (LANES, LANES), 0)
    lane_iota = lax.broadcasted_iota(jnp.int32, (LANES, LANES), 1)
    for r in range(stage.shape[0] // LANES):
        got = stage[r * LANES : (r + 1) * LANES, :]
        pieces = jnp.concatenate([got >> 16, (got >> 8) & 255, got & 255], axis=0)
        pieces = pieces.astype(jnp.float32).astype(jnp.bfloat16)
        low = ids_ref[pl.ds(first + r, 1), :] & (LANES - 1)
        hot = (sub_iota == low).astype(jnp.float32).astype(jnp.bfloat16)
        found = dot_nn(pieces, hot)
        found = found[:LANES] * 65536.0 + found[LANES : 2 * LANES] * 256.0 + found[2 * LANES :]
        picked = jnp.sum(jnp.where(sub_iota == lane_iota, found, 0.0), axis=0, keepdims=True)
        pos_ref[pl.ds(first + r, 1), :] = picked.astype(jnp.int32)


def lookup_step(step, ids_ref, smem_ref, map_ref, stage_a, stage_b, pos_ref):
    first = step * 4
    gather_map(first, smem_ref, map_ref, stage_a)

    pick_lanes(first, ids_ref, stage_a, pos_ref)
    gather_map(first + 2, smem_ref, map_ref, stage_b)
    pick_lanes(first + 2, ids_ref, stage_b, pos_ref)


def assign(pos_ref, own_ref, val_ref, slot_ref, addr_ref, req_ref, *, parts, shift, cap_row):
    rows = pos_ref.shape[0]
    position = pos_ref[...]
    owner = position >> shift
    local = position & ((1 << shift) - 1)
    row_iota = lax.broadcasted_iota(jnp.int32, (rows, LANES), 0)
    is_cold = (local >= HOT_DEV) & (row_iota < ID_ROWS)
    own_ref[...] = jnp.where(is_cold, owner, -1)
    val_ref[...] = local
    part_iota = lax.broadcasted_iota(jnp.int32, (parts, LANES), 0)
    slot_iota = lax.broadcasted_iota(jnp.int32, (LANES, LANES), 0)
    upper = lax.broadcasted_iota(jnp.int32, (LANES, 2 * LANES), 0) <= lax.broadcasted_iota(
        jnp.int32, (LANES, 2 * LANES), 1
    )
    upper = upper.astype(jnp.float32).astype(jnp.bfloat16)

    def block(step, carry):
        base, table = carry
        at = pl.ds(pl.multiple_of(step * 8, 8), 8)
        own8 = own_ref[at, :]
        val8 = val_ref[at, :].astype(jnp.float32)
        top8 = jnp.floor(val8 * (1.0 / LANES))
        low8 = val8 - top8 * LANES
        slots, lefts = [], []
        for q in range(8):
            mine = part_iota == own8[q : q + 1, :]
            counts = dot_nn(mine.astype(jnp.float32).astype(jnp.bfloat16), upper)
            slots.append(jnp.sum(jnp.where(mine, counts[:, :LANES] + base, 0.0), axis=0, keepdims=True) - 1.0)
            base = base + counts[:, LANES:]
            lefts.append(
                jnp.concatenate(
                    [jnp.where(mine, top8[q : q + 1, :], 0.0), jnp.where(mine, low8[q : q + 1, :], 0.0)], axis=0
                ).astype(jnp.bfloat16)
            )
        slot8 = jnp.concatenate(slots, axis=0).astype(jnp.int32)
        slot_ref[at, :] = slot8
        for q in range(0, 8, 2):
            rights = [
                (slot_iota == slot8[k : k + 1, :]).astype(jnp.float32).astype(jnp.bfloat16) for k in (q, q + 1)
            ]
            table = table + dot_nt(
                jnp.concatenate([lefts[q], lefts[q + 1]], axis=1), jnp.concatenate(rights, axis=1)
            )
        return base, table

    start = (jnp.zeros((parts, LANES), jnp.float32), jnp.zeros((2 * parts, LANES), jnp.float32))
    table = lax.fori_loop(0, rows // 8, block, start)[1]
    request = (table[:parts] * LANES + table[parts:]).astype(jnp.int32) & ((1 << shift) - 1)
    for p in range(parts):
        req_ref[p, 0:1, :] = request[p : p + 1, :]
    hot_addr = (owner & 1) * (HUB_ROWS // 2) + (owner >> 1) * HOT_DEV + (local & (HOT_DEV - 1))
    addr = jnp.where(is_cold, HUB_ROWS + owner * cap_row + slot_ref[...], hot_addr)
    addr_ref[...] = jnp.clip(addr, 0, HUB_ROWS + parts * cap_row - 1)


def tree_sum(values):
    while len(values) > 1:
        values = [a + b for a, b in zip(values[::2], values[1::2])] + (
            [values[-1]] if len(values) % 2 else []
        )
    return values[0]


def fetch_rows(addr_smem, wide, own_buf, far_buf, x_ref, *, seeds, fan_one, fan_two):
    hops = seeds * fan_one
    feat = wide.shape[1]
    half = fan_two // 2
    top = half * fan_one

    def fetch(step, carry):
        j = step // (seeds // 8)
        seed = lax.rem(step, seeds // 8) * 8
        base = pl.multiple_of(step * 8, 8)
        late = j // 8
        own_row = top + j - 8 * late
        for k in range(8):
            own_buf[pl.ds(base + k, 1), :] = wide[pl.ds(addr_smem[own_row, late * seeds + seed + k], 1), :]
            rows = [
                wide[pl.ds(addr_smem[m % half * fan_one + j, m // half * seeds + seed + k], 1), :]
                for m in range(fan_two)
            ]
            far_buf[pl.ds(base + k, 1), :] = tree_sum(rows)
        return carry

    lax.fori_loop(0, hops // 8, fetch, 0)

    def fetch_seed(step, carry):
        base = pl.multiple_of(step * 8, 8)
        for k in range(8):
            own_buf[pl.ds(hops + base + k, 1), :] = wide[
                pl.ds(addr_smem[top + fan_one - 8, seeds + base + k], 1), :
            ]
        return carry

    lax.fori_loop(0, seeds // 8, fetch_seed, 0)
    row_sum = jnp.zeros((seeds, feat), jnp.float32)
    for j in range(fan_one):
        at = slice(j * seeds, (j + 1) * seeds)
        own = own_buf[at, :]
        row_sum = row_sum + own
        x_ref[at, :feat] = own.astype(jnp.bfloat16)
        x_ref[at, feat:] = (far_buf[at, :] * (1.0 / fan_two)).astype(jnp.bfloat16)
    x_ref[hops:, :feat] = own_buf[hops:, :].astype(jnp.bfloat16)
    x_ref[hops:, feat:] = (row_sum * (1.0 / fan_one)).astype(jnp.bfloat16)


def front_kernel(
    hop2_ref, hop1_ref, seed_ref, map_hbm, feat_hbm,
    table_ref, addr_ref,
    ids_ref, pos_ref, own_ref, val_ref, slot_ref, map_ref, feat_ref, wide, stage_a, stage_b, row_stage,
    req_ref, inbox, send, ids_smem, wanted,
    local_sem, req_send, req_recv, hub_send, hub_recv, row_send, row_recv, *, parts, shift, cap_row,
):
    node_rows = feat_ref.shape[0]
    me = lax.axis_index("dom")
    core, z, x = lax.rem(me, 2), lax.rem(me // 2, N_Z), me // (2 * N_Z)
    barrier = pltpu.get_barrier_semaphore()

    get_map = pltpu.make_async_copy(map_hbm, map_ref, local_sem.at[0])
    get_map.start()
    get_feat = pltpu.make_async_copy(feat_hbm, feat_ref, local_sem.at[1])
    get_feat.start()
    x_rows = N_Z * HOT_DEV
    half = N_X * x_rows
    own_at = pl.ds(pl.multiple_of(core * half + (x * N_Z + z) * HOT_DEV, HOT_DEV), HOT_DEV)
    keep_hub = pltpu.make_async_copy(feat_hbm.at[pl.ds(0, HOT_DEV)], table_ref.at[own_at], local_sem.at[2])
    keep_hub.start()

    def peer(step):
        k = lax.rem(step, 8)
        dz = lax.rem(N_Z + 4 + (lax.rem(k, 2) * 2 - 1) * ((k + 1) // 2), N_Z)
        dxc = lax.rem(step // 8 + 1, 8)
        other = (lax.rem(x + dxc // 2, N_X) * N_Z + lax.rem(z + dz, N_Z)) * 2 + lax.rem(core + lax.rem(dxc, 2), 2)
        return other, {"dom": other}

    def greet(step, carry):
        pl.semaphore_signal(barrier, inc=1, device_id=peer(step)[1], device_id_type=MESH)
        return carry

    lax.fori_loop(0, parts - 1, greet, 0)

    place_ids(hop2_ref, hop1_ref, seed_ref, ids_ref)
    ids_down = pltpu.make_async_copy(ids_ref, ids_smem, local_sem.at[3])
    ids_down.start()
    get_feat.wait()

    def widen(step, carry):
        at = pl.ds(pl.multiple_of(step * 64, 64), 64)
        wide[at, :] = feat_ref[at, :].astype(jnp.float32)
        return carry

    lax.fori_loop(0, node_rows // 64, widen, 0)
    keep_hub.wait()

    def hub_copy(at, level, where):
        return pltpu.make_async_remote_copy(
            table_ref.at[at], table_ref.at[at], hub_send.at[level], hub_recv.at[level],
            device_id=where, device_id_type=MESH,
        )

    def hub_wait(rows, level):
        return hub_copy(pl.ds(0, rows), level, peer(0)[1])

    def send_z(step, carry):
        hub_copy(own_at, 0, {"dom": (x * N_Z + lax.rem(z + step, N_Z)) * 2 + core}).start()
        return carry

    def x_at(step):
        return pl.ds(pl.multiple_of(core * half + lax.rem(x + step, N_X) * x_rows, x_rows), x_rows)

    def send_x(step, carry):
        hub_copy(x_at(0), 1, {"dom": (lax.rem(x + step, N_X) * N_Z + z) * 2 + core}).start()
        return carry

    def send_core(step, carry):
        hub_copy(x_at(step), 2, {"dom": me + 1 - 2 * core}).start()
        return carry

    get_map.wait()
    ids_down.wait()

    def lookup(step, carry):
        lookup_step(step, ids_ref, ids_smem, map_ref, stage_a, stage_b, pos_ref)
        return carry

    groups = -(-ID_ROWS // 4)
    lax.fori_loop(0, groups // 3, lookup, 0)
    pl.semaphore_wait(barrier, parts - 1)
    lax.fori_loop(1, N_Z, send_z, 0)
    lax.fori_loop(groups // 3, groups, lookup, 0)
    hub_wait((N_Z - 1) * HOT_DEV, 0).wait_recv()
    lax.fori_loop(1, N_X, send_x, 0)
    lax.fori_loop(0, 1, send_core, 0)
    for r in range(groups * 4, pos_ref.shape[0]):
        pos_ref[r : r + 1, :] = jnp.zeros((1, LANES), jnp.int32)
    assign(
        pos_ref, own_ref, val_ref, slot_ref, addr_ref, req_ref, parts=parts, shift=shift, cap_row=cap_row,
    )
    ask_at = pl.ds(0, 1)
    keep_req = pltpu.make_async_copy(req_ref.at[me], inbox.at[me], local_sem.at[4])
    keep_req.start()

    def ask(step, carry):
        other, where = peer(step)
        pltpu.make_async_remote_copy(
            req_ref.at[other, ask_at], inbox.at[me, ask_at], req_send, req_recv, device_id=where, device_id_type=MESH
        ).start()
        return carry

    lax.fori_loop(0, parts - 1, ask, 0)
    most = pl.ds(0, parts - 1)
    asked = pltpu.make_async_remote_copy(
        req_ref.at[most, ask_at], inbox.at[most, ask_at], req_send, req_recv,
        device_id=peer(0)[1], device_id_type=MESH,
    )
    keep_req.wait()
    asked.wait_recv()
    to_scalar = pltpu.make_async_copy(inbox.at[:, ask_at], wanted, local_sem.at[5])
    to_scalar.start()
    to_scalar.wait()

    def collect(other):
        for i in range(cap_row):
            row_stage[i : i + 1, :] = wide[pl.ds(wanted[other, 0, i], 1), :]
        return row_stage[...].astype(jnp.bfloat16)

    def rows_at(part):
        return pl.ds(pl.multiple_of(HUB_ROWS + part * cap_row, 8), cap_row)

    def serve(step, carry):
        other, where = peer(step)
        send[other] = collect(other)
        pltpu.make_async_remote_copy(
            send.at[other], table_ref.at[rows_at(me)], row_send, row_recv, device_id=where, device_id_type=MESH
        ).start()
        return carry

    lax.fori_loop(0, parts - 1, serve, 0)
    table_ref[rows_at(me), :] = collect(me)
    hub_wait((N_X - 1) * x_rows, 1).wait_recv()
    lax.fori_loop(1, N_X, send_core, 0)

    asked.wait_send()
    hub_wait((N_Z - 1) * HOT_DEV, 0).wait_send()
    hub_wait((N_X - 1) * x_rows, 1).wait_send()
    hub_wait(half, 2).wait()
    pltpu.make_async_remote_copy(
        send.at[most], send.at[most], row_send, row_recv, device_id=peer(0)[1], device_id_type=MESH
    ).wait()


def front(hop2, hop1, seed_ids, partition_map, features, cap_row):
    parts = lax.axis_size("dom")
    node_rows, feat = features.shape
    vmem = pl.BlockSpec(memory_space=pltpu.VMEM)
    hbm = pl.BlockSpec(memory_space=pltpu.HBM)
    rows = round_up(ID_ROWS, 8)
    table_rows = HUB_ROWS + parts * cap_row
    return pl.pallas_call(
        functools.partial(front_kernel, parts=parts, shift=node_rows.bit_length() - 1, cap_row=cap_row),
        name="front",
        out_shape=(
            jax.ShapeDtypeStruct((table_rows, feat), features.dtype),
            jax.ShapeDtypeStruct((rows, LANES), jnp.int32),
        ),
        in_specs=[vmem, vmem, vmem, hbm, hbm],
        out_specs=(vmem, vmem),
        scratch_shapes=[pltpu.VMEM((rows, LANES), jnp.int32)] * 5
        + [
            pltpu.VMEM((partition_map.size // LANES, LANES), jnp.int32),
            pltpu.VMEM((node_rows, feat), features.dtype),
            pltpu.VMEM((node_rows, feat), jnp.float32),
            pltpu.VMEM((2 * LANES, LANES), jnp.int32),
            pltpu.VMEM((2 * LANES, LANES), jnp.int32),
            pltpu.VMEM((cap_row, feat), jnp.float32),
            pltpu.VMEM((parts, 8, LANES), jnp.int32),
            pltpu.VMEM((parts, 8, LANES), jnp.int32),
            pltpu.VMEM((parts, cap_row, feat), features.dtype),
            pltpu.SMEM((rows, LANES), jnp.int32),
            pltpu.SMEM((parts, 1, LANES), jnp.int32),
            pltpu.SemaphoreType.DMA((6,)),
            pltpu.SemaphoreType.DMA,
            pltpu.SemaphoreType.DMA,
            pltpu.SemaphoreType.DMA((3,)),
            pltpu.SemaphoreType.DMA((3,)),
            pltpu.SemaphoreType.DMA,
            pltpu.SemaphoreType.DMA,
        ],
        compiler_params=pltpu.CompilerParams(collective_id=2, has_side_effects=True, vmem_limit_bytes=24 * MIB),
    )(hop2, hop1, seed_ids.reshape(1, -1), partition_map.reshape(-1, LANES), features)

def fetch_kernel(addr_smem, table_ref, x_ref, table_wide, own_buf, far_buf, *, seeds, fan_one, fan_two):
    def widen(step, carry):
        at = pl.ds(pl.multiple_of(step * 128, 128), 128)
        table_wide[at, :] = table_ref[at, :].astype(jnp.float32)
        return carry

    lax.fori_loop(0, table_ref.shape[0] // 128, widen, 0)
    fetch_rows(addr_smem, table_wide, own_buf, far_buf, x_ref, seeds=seeds, fan_one=fan_one, fan_two=fan_two)


def fetch_all(addr, table, seeds, fan_one, fan_two):
    feat = table.shape[1]
    total = seeds * (1 + fan_one)
    vmem = pl.BlockSpec(memory_space=pltpu.VMEM)
    return pl.pallas_call(
        functools.partial(fetch_kernel, seeds=seeds, fan_one=fan_one, fan_two=fan_two),
        name="fetch",
        out_shape=jax.ShapeDtypeStruct((total, 2 * feat), table.dtype),
        in_specs=[pl.BlockSpec(memory_space=pltpu.SMEM), vmem],
        out_specs=vmem,
        scratch_shapes=[
            pltpu.VMEM(table.shape, jnp.float32),
            pltpu.VMEM((total, feat), jnp.float32),
            pltpu.VMEM((total, feat), jnp.float32),
        ],
        compiler_params=pltpu.CompilerParams(vmem_limit_bytes=24 * MIB),
    )(addr, table)


ROOT = 0.7978845608028654
CUBE = 0.044715


def gelu_pair(pre):
    square = pre * pre
    bend = jnp.tanh(ROOT * pre * (1.0 + CUBE * square))
    half = 0.5 * (1.0 + bend)
    slope = half + 0.5 * pre * (1.0 - bend * bend) * (ROOT * (1.0 + 3.0 * CUBE * square))
    return pre * half, slope


N_REP = 4
MEMBERS = N_X * N_REP * 2
PART_TWO = 24
PART_ONE = 16
PART = PART_TWO + PART_ONE
HIGH = 176


def pack_two(part_ref, g_two, gb_two):
    classes, width = g_two.shape
    for h in range(width // LANES):
        for b in range(HIGH // 8):
            block = h * (HIGH // 8) + b
            to = block % 3 * 8
            rows = min(8, classes - b * 8)
            part_ref[block // 3, to : to + rows, :] = g_two[
                b * 8 : b * 8 + rows, h * LANES : (h + 1) * LANES
            ].astype(jnp.bfloat16)
            if rows < 8:
                part_ref[block // 3, to + rows : to + 8, :] = jnp.zeros((8 - rows, LANES), jnp.bfloat16)
    first = width // LANES * (HIGH // 8)
    for block in range(first, MEMBERS * 3):
        to = block % 3 * 8
        part_ref[block // 3, to : to + 8, :] = jnp.zeros((8, LANES), jnp.bfloat16)
    to = first % 3 * 8
    part_ref[first // 3, to : to + 1, :] = gb_two[:, :LANES].astype(jnp.bfloat16)
    part_ref[first // 3, to + 1 : to + 2, : classes - LANES] = gb_two[:, LANES:].astype(jnp.bfloat16)


def pack_one(part_ref, g_one, gb_one):
    halves = g_one.shape[1] // LANES
    each = g_one.shape[0] // PART_ONE
    for h in range(halves):
        for i in range(each):
            part_ref[h * each + i, PART_TWO:, :] = g_one[
                i * PART_ONE : (i + 1) * PART_ONE, h * LANES : (h + 1) * LANES
            ].astype(jnp.bfloat16)
        part_ref[MEMBERS - 1, 16 + h : 17 + h, :] = gb_one[:, h * LANES : (h + 1) * LANES].astype(jnp.bfloat16)


def dense_kernel(
    x_ref, label_ref, self_one, neigh_one, b_one_ref, self_two, neigh_two, b_two_ref,
    loss_ref, gathered,
    slope_buf, d_buf, part_ref, box, z_box, send_sem, recv_sem, *, seeds, fan_one,
):
    hidden = self_one.shape[1]
    hops = seeds * fan_one
    me, y = lax.axis_index("dom"), lax.axis_index("rep")
    core, z, x = lax.rem(me, 2), lax.rem(me // 2, N_Z), me // (2 * N_Z)
    mine = (x * N_REP + y) * 2 + core
    barrier = pltpu.get_barrier_semaphore()

    def spread(k, size):
        return lax.rem(size + size // 2 + (lax.rem(k, 2) * 2 - 1) * ((k + 1) // 2), size)

    def near(step):
        other_x = lax.rem(x + spread(step // 8, N_X), N_X)
        other_y = lax.rem(y + spread(lax.rem(step // 2, N_REP), N_REP), N_REP)
        other_core = lax.rem(core + lax.rem(step + 1, 2), 2)
        where = {"dom": (other_x * N_Z + z) * 2 + other_core, "rep": other_y}
        return (other_x * N_REP + other_y) * 2 + other_core, where

    def far(step):
        return {"dom": (x * N_Z + lax.rem(z + spread(step, N_Z), N_Z)) * 2 + core, "rep": y}

    def greet_near(step, carry):
        pl.semaphore_signal(barrier, inc=1, device_id=near(step)[1], device_id_type=MESH)
        return carry

    def greet_far(step, carry):
        pl.semaphore_signal(barrier, inc=1, device_id=far(step), device_id_type=MESH)
        return carry

    lax.fori_loop(0, N_Z - 1, greet_far, 0)
    lax.fori_loop(0, MEMBERS - 1, greet_near, 0)

    w_one = jnp.concatenate([self_one[...], neigh_one[...]], axis=0)
    w_two = jnp.concatenate([self_two[...], neigh_two[...]], axis=1)
    b_one = b_one_ref[...]
    hid_sum = jnp.zeros((seeds, hidden), jnp.float32)
    act = None
    for j in range(fan_one + 1):
        at = slice(j * seeds, (j + 1) * seeds)
        act, slope = gelu_pair(dot_nn(x_ref[at, :], w_one) + b_one)
        act = act.astype(jnp.bfloat16)
        slope_buf[at, :] = slope
        if j < fan_one:
            hid_sum = hid_sum + act.astype(jnp.float32)
    hid = jnp.concatenate([act, (hid_sum * (1.0 / fan_one)).astype(jnp.bfloat16)], axis=1)
    logits = dot_nt(hid, w_two) + b_two_ref[...]
    shifted = logits - jnp.max(logits, axis=1, keepdims=True)
    log_probs = shifted - jnp.log(jnp.sum(jnp.exp(shifted), axis=1, keepdims=True))
    class_iota = lax.broadcasted_iota(jnp.int32, logits.shape, 1)
    diagonal = lax.broadcasted_iota(jnp.int32, (seeds, seeds), 0) == lax.broadcasted_iota(jnp.int32, (seeds, seeds), 1)
    label = jnp.sum(jnp.where(diagonal, label_ref[...].astype(jnp.float32), 0.0), axis=1, keepdims=True)
    target = (class_iota.astype(jnp.float32) == label).astype(jnp.float32)
    loss = jnp.sum(log_probs * target, axis=1, keepdims=True)
    loss_ref[...] = -jnp.sum(jnp.where(diagonal, loss, 0.0), axis=0, keepdims=True)
    d_logits = ((jnp.exp(log_probs) - target) * (1.0 / seeds)).astype(jnp.bfloat16)
    pack_two(part_ref, dot_tn(d_logits, hid), jnp.sum(d_logits.astype(jnp.float32), axis=0, keepdims=True))
    pl.semaphore_wait(barrier, MEMBERS + N_Z - 2)

    def copy(source, target, stage, where):
        return pltpu.make_async_remote_copy(
            source, target, send_sem.at[stage], recv_sem.at[stage], device_id=where, device_id_type=MESH
        )

    two_at, one_at = pl.ds(0, PART_TWO), pl.ds(PART_TWO, PART_ONE)

    def send_two(step, carry):
        other, where = near(step)

        @pl.when(other < MEMBERS - 1)
        def _():
            copy(part_ref.at[other, two_at], box.at[mine, two_at], 0, where).start()

        return carry

    lax.fori_loop(0, MEMBERS - 1, send_two, 0)
    d_hid = dot_nn(d_logits, w_two)
    d_hop = d_hid[:, hidden:] * (1.0 / fan_one)
    for j in range(fan_one + 1):
        at = slice(j * seeds, (j + 1) * seeds)
        d_pre = ((d_hop if j < fan_one else d_hid[:, :hidden]) * slope_buf[at, :]).astype(jnp.bfloat16)
        d_buf[at, :] = d_pre
    gb_one = dot_nn(jnp.ones((8, d_buf.shape[0]), jnp.bfloat16), d_buf[...])[:1]
    pack_one(part_ref, dot_tn(x_ref[...], d_buf[...]), gb_one)

    def send_one(step, carry):
        other, where = near(step)
        copy(part_ref.at[other, one_at], box.at[mine, one_at], 0, where).start()

        @pl.when(other == MEMBERS - 1)
        def _():
            copy(part_ref.at[other, two_at], box.at[mine, two_at], 0, where).start()

        return carry

    lax.fori_loop(0, MEMBERS - 1, send_one, 0)
    box[mine] = part_ref[mine]
    some = box.at[pl.ds(0, MEMBERS - 1)]
    first = copy(some, some, 0, near(0)[1])
    first.wait_recv()
    total = box[0].astype(jnp.float32)
    for i in range(1, MEMBERS):
        total = total + box[i].astype(jnp.float32)
    z_box[z] = total

    def across(step, carry):
        copy(z_box.at[z], z_box.at[z], 1, far(step)).start()
        return carry

    lax.fori_loop(0, N_Z - 1, across, 0)
    some = z_box.at[pl.ds(0, N_Z - 1)]
    second = copy(some, some, 1, far(0))
    second.wait_recv()
    total = z_box[0]
    for i in range(1, N_Z):
        total = total + z_box[i]
    gathered[mine] = total.astype(jnp.bfloat16)

    def back(step, carry):
        copy(gathered.at[mine], gathered.at[mine], 2, near(step)[1]).start()
        return carry

    lax.fori_loop(0, MEMBERS - 1, back, 0)
    some = gathered.at[pl.ds(0, MEMBERS - 1)]
    third = copy(some, some, 2, near(0)[1])
    third.wait_recv()
    first.wait_send()
    second.wait_send()
    third.wait_send()


def dense(x, labels, self_one, neigh_one, bias_one, self_two, neigh_two, bias_two, fan_one):
    seeds = labels.shape[0]
    hidden = self_one.shape[1]
    classes = self_two.shape[1]
    total = x.shape[0]
    vmem = pl.BlockSpec(memory_space=pltpu.VMEM)
    return pl.pallas_call(
        functools.partial(dense_kernel, seeds=seeds, fan_one=fan_one),
        name="dense",
        out_shape=(
            jax.ShapeDtypeStruct((1, seeds), jnp.float32),
            jax.ShapeDtypeStruct((MEMBERS, PART, LANES), jnp.bfloat16),
        ),
        in_specs=[vmem] * 8,
        out_specs=(vmem,) * 2,
        scratch_shapes=[
            pltpu.VMEM((total, hidden), jnp.float32),
            pltpu.VMEM((total, hidden), jnp.bfloat16),
            pltpu.VMEM((MEMBERS, PART, LANES), jnp.bfloat16),
            pltpu.VMEM((MEMBERS, PART, LANES), jnp.bfloat16),
            pltpu.VMEM((N_Z, PART, LANES), jnp.float32),
            pltpu.SemaphoreType.DMA((3,)),
            pltpu.SemaphoreType.DMA((3,)),
        ],
        compiler_params=pltpu.CompilerParams(collective_id=1, has_side_effects=True, vmem_limit_bytes=16 * MIB),
    )(
        x,
        labels.reshape(1, seeds),
        self_one,
        neigh_one,
        bias_one.reshape(1, hidden),
        self_two.T,
        neigh_two.T,
        bias_two.reshape(1, classes),
    )


def unpack_kernel(gathered, loss_in, loss_out, self_one, neigh_one, bias_one, self_two, neigh_two, bias_two):
    feat, hidden = self_one.shape
    classes = self_two.shape[0]
    loss_out[...] = loss_in[...]
    halves = hidden // LANES
    each = feat // PART_ONE
    for h in range(halves):
        cols = slice(h * LANES, (h + 1) * LANES)
        for i in range(each):
            at = slice(i * PART_ONE, (i + 1) * PART_ONE)
            self_one[at, cols] = gathered[h * 2 * each + i, PART_TWO:, :].astype(jnp.float32)
            neigh_one[at, cols] = gathered[h * 2 * each + each + i, PART_TWO:, :].astype(jnp.float32)
        for b in range(HIGH // 8):
            rows = min(8, classes - b * 8)
            for k, out in enumerate((self_two, neigh_two)):
                block = (k * halves + h) * (HIGH // 8) + b
                to = block % 3 * 8
                out[b * 8 : b * 8 + rows, cols] = gathered[block // 3, to : to + 8, :].astype(jnp.float32)[:rows]
        bias_one[:, cols] = gathered[MEMBERS - 1, 16:24, :].astype(jnp.float32)[h : h + 1]
    first = 2 * halves * (HIGH // 8)
    to = first % 3 * 8
    last = gathered[first // 3, to : to + 8, :].astype(jnp.float32)
    bias_two[:, :LANES] = last[:1]
    bias_two[:, LANES:] = last[1:2, : classes - LANES]


def unpack(gathered, loss, feat, hidden, classes):
    vmem = pl.BlockSpec(memory_space=pltpu.VMEM)
    shapes = [loss.shape, (feat, hidden), (feat, hidden), (1, hidden), (classes, hidden), (classes, hidden), (1, classes)]
    return pl.pallas_call(
        unpack_kernel,
        name="unpack",
        out_shape=tuple(jax.ShapeDtypeStruct(shape, jnp.float32) for shape in shapes),
        in_specs=[vmem] * 2,
        out_specs=(vmem,) * 7,
        compiler_params=pltpu.CompilerParams(vmem_limit_bytes=8 * MIB),
    )(gathered, loss)


def shards(
    features, partition_map, seed_ids, hop1_ids, hop2_ids, labels,
    self_one, neigh_one, bias_one, self_two, neigh_two, bias_two,
):
    parts = lax.axis_size("dom")
    seeds = seed_ids.shape[0]
    fan_one = hop1_ids.shape[1]
    fan_two = hop2_ids.shape[2]
    feat = features.shape[1]
    tree_rows = 1 + fan_one + fan_one * fan_two
    cold_cap = tree_rows // 2 * (seeds // parts)
    cap_row = round_up(cold_cap, 8)
    table, addr = front(hop2_ids.transpose(2, 1, 0), hop1_ids.T, seed_ids, partition_map, features, cap_row)
    x = fetch_all(addr, table, seeds, fan_one, fan_two)
    hidden, classes = self_two.shape
    loss, gathered = dense(x, labels, self_one, neigh_one, bias_one, self_two, neigh_two, bias_two, fan_one)
    loss, *grads = unpack(gathered, loss, feat, hidden, classes)
    return (
        loss.reshape(-1), grads[0], grads[1], grads[2].reshape(-1),
        grads[3].T, grads[4].T, grads[5].reshape(-1),
    )


def solution(mesh):
    return jax.shard_map(
        shards,
        mesh=mesh,
        in_specs=(
            P("dom", None),
            P(),
            P(("dom", "rep")),
            P(("dom", "rep"), None),
            P(("dom", "rep"), None, None),
            P(("dom", "rep")),
            P(),
            P(),
            P(),
            P(),
            P(),
            P(),
        ),
        out_specs=(P(("dom", "rep")), P(), P(), P(), P(), P(), P()),
        check_vma=False,
    )
```

```python
import functools

import jax
import jax.numpy as jnp
from jax import lax
from jax.experimental import pallas as pl
from jax.experimental.pallas import tpu as pltpu
from jax.sharding import PartitionSpec as P

HOT_DEV = 256
LANES = 128
MESH = pl.DeviceIdType.MESH
MIB = 1024 * 1024


def round_up(value, unit):
    return -(-value // unit) * unit


def dot_tn(left, right):
    return lax.dot_general(left, right, (((0,), (0,)), ((), ())), preferred_element_type=jnp.float32)


def dot_nt(left, right):
    return lax.dot_general(left, right, (((1,), (1,)), ((), ())), preferred_element_type=jnp.float32)


def dot_nn(left, right):
    return jnp.dot(left, right, preferred_element_type=jnp.float32)


N_X, N_Z = 4, 8
ID_ROWS = 83
HUB_ROWS = 64 * HOT_DEV


def place_ids(hop2_ref, hop1_ref, seed_ref, ids_ref):
    fan_two, fan_one, seeds = hop2_ref.shape
    half = fan_two // 2
    ids_ref[...] = jnp.zeros(ids_ref.shape, jnp.int32)
    for m in range(half):
        at = slice(m * fan_one, (m + 1) * fan_one)
        ids_ref[at, :seeds] = hop2_ref[m]
        ids_ref[at, seeds:] = hop2_ref[half + m]
    top = half * fan_one
    ids_ref[top : top + 8, :seeds] = hop1_ref[:8, :]
    ids_ref[top : top + fan_one - 8, seeds:] = hop1_ref[8:, :]
    ids_ref[top + fan_one - 8 : top + fan_one - 7, seeds:] = seed_ref[...]


def gather_map(first, smem_ref, map_ref, stage):
    for r in range(stage.shape[0] // LANES):
        high = smem_ref.at[first + r]
        for i in range(LANES):
            stage[r * LANES + i : r * LANES + i + 1, :] = map_ref[pl.ds(high[i], 1), :]


def pick_lanes(first, ids_ref, stage, pos_ref):
    sub_iota = lax.broadcasted_iota(jnp.int32, (LANES, LANES), 0)
    lane_iota = lax.broadcasted_iota(jnp.int32, (LANES, LANES), 1)
    for r in range(stage.shape[0] // LANES):
        got = stage[r * LANES : (r + 1) * LANES, :]
        pieces = jnp.concatenate([got >> 16, (got >> 8) & 255, got & 255], axis=0)
        pieces = pieces.astype(jnp.float32).astype(jnp.bfloat16)
        low = ids_ref[pl.ds(first + r, 1), :] & (LANES - 1)
        hot = (sub_iota == low).astype(jnp.float32).astype(jnp.bfloat16)
        found = dot_nn(pieces, hot)
        found = found[:LANES] * 65536.0 + found[LANES : 2 * LANES] * 256.0 + found[2 * LANES :]
        picked = jnp.sum(jnp.where(sub_iota == lane_iota, found, 0.0), axis=0, keepdims=True)
        pos_ref[pl.ds(first + r, 1), :] = picked.astype(jnp.int32)


def lookup_step(step, ids_ref, smem_ref, map_ref, stage_a, stage_b, pos_ref):
    first = step * 4
    gather_map(first, smem_ref, map_ref, stage_a)

    pick_lanes(first, ids_ref, stage_a, pos_ref)
    gather_map(first + 2, smem_ref, map_ref, stage_b)
    pick_lanes(first + 2, ids_ref, stage_b, pos_ref)


def assign(pos_ref, own_ref, val_ref, slot_ref, addr_ref, req_ref, *, parts, shift, cap_row):
    rows = pos_ref.shape[0]
    position = pos_ref[...]
    owner = position >> shift
    local = position & ((1 << shift) - 1)
    row_iota = lax.broadcasted_iota(jnp.int32, (rows, LANES), 0)
    is_cold = (local >= HOT_DEV) & (row_iota < ID_ROWS)
    own_ref[...] = jnp.where(is_cold, owner, -1)
    val_ref[...] = local
    part_iota = lax.broadcasted_iota(jnp.int32, (parts, LANES), 0)
    slot_iota = lax.broadcasted_iota(jnp.int32, (LANES, LANES), 0)
    upper = lax.broadcasted_iota(jnp.int32, (LANES, 2 * LANES), 0) <= lax.broadcasted_iota(
        jnp.int32, (LANES, 2 * LANES), 1
    )
    upper = upper.astype(jnp.float32).astype(jnp.bfloat16)

    def block(step, carry):
        base, table = carry
        at = pl.ds(pl.multiple_of(step * 8, 8), 8)
        own8 = own_ref[at, :]
        val8 = val_ref[at, :].astype(jnp.float32)
        top8 = jnp.floor(val8 * (1.0 / LANES))
        low8 = val8 - top8 * LANES
        slots, lefts = [], []
        for q in range(8):
            mine = part_iota == own8[q : q + 1, :]
            counts = dot_nn(mine.astype(jnp.float32).astype(jnp.bfloat16), upper)
            slots.append(jnp.sum(jnp.where(mine, counts[:, :LANES] + base, 0.0), axis=0, keepdims=True) - 1.0)
            base = base + counts[:, LANES:]
            lefts.append(
                jnp.concatenate(
                    [jnp.where(mine, top8[q : q + 1, :], 0.0), jnp.where(mine, low8[q : q + 1, :], 0.0)], axis=0
                ).astype(jnp.bfloat16)
            )
        slot8 = jnp.concatenate(slots, axis=0).astype(jnp.int32)
        slot_ref[at, :] = slot8
        for q in range(0, 8, 2):
            rights = [
                (slot_iota == slot8[k : k + 1, :]).astype(jnp.float32).astype(jnp.bfloat16) for k in (q, q + 1)
            ]
            table = table + dot_nt(
                jnp.concatenate([lefts[q], lefts[q + 1]], axis=1), jnp.concatenate(rights, axis=1)
            )
        return base, table

    start = (jnp.zeros((parts, LANES), jnp.float32), jnp.zeros((2 * parts, LANES), jnp.float32))
    table = lax.fori_loop(0, rows // 8, block, start)[1]
    request = (table[:parts] * LANES + table[parts:]).astype(jnp.int32) & ((1 << shift) - 1)
    for p in range(parts):
        req_ref[p, 0:1, :] = request[p : p + 1, :]
    hot_addr = (owner & 1) * (HUB_ROWS // 2) + (owner >> 1) * HOT_DEV + (local & (HOT_DEV - 1))
    addr = jnp.where(is_cold, HUB_ROWS + owner * cap_row + slot_ref[...], hot_addr)
    addr_ref[...] = jnp.clip(addr, 0, HUB_ROWS + parts * cap_row - 1)


def tree_sum(values):
    while len(values) > 1:
        values = [a + b for a, b in zip(values[::2], values[1::2])] + (
            [values[-1]] if len(values) % 2 else []
        )
    return values[0]


def fetch_rows(addr_smem, wide, own_buf, far_buf, x_ref, *, seeds, fan_one, fan_two):
    hops = seeds * fan_one
    feat = wide.shape[1]
    half = fan_two // 2
    top = half * fan_one

    def fetch(j, carry):
        late = j // 8
        own_at = addr_smem.at[top + j - 8 * late, pl.ds(pl.multiple_of(late * seeds, seeds), seeds)]
        far_at = [addr_smem.at[m * fan_one + j] for m in range(half)]
        base = pl.multiple_of(j * seeds, seeds)
        own_out, far_out = own_buf.at[pl.ds(base, seeds)], far_buf.at[pl.ds(base, seeds)]
        for k in range(seeds):
            own_out[k : k + 1, :] = wide[pl.ds(own_at[k], 1), :]
            rows = [wide[pl.ds(far_at[m % half][m // half * seeds + k], 1), :] for m in range(fan_two)]
            far_out[k : k + 1, :] = tree_sum(rows)
        return carry

    lax.fori_loop(0, fan_one, fetch, 0)

    def fetch_seed(step, carry):
        base = pl.multiple_of(step * 8, 8)
        for k in range(8):
            own_buf[pl.ds(hops + base + k, 1), :] = wide[
                pl.ds(addr_smem[top + fan_one - 8, seeds + base + k], 1), :
            ]
        return carry

    lax.fori_loop(0, seeds // 8, fetch_seed, 0)
    row_sum = jnp.zeros((seeds, feat), jnp.float32)
    for j in range(fan_one):
        at = slice(j * seeds, (j + 1) * seeds)
        own = own_buf[at, :]
        row_sum = row_sum + own
        x_ref[at, :feat] = own.astype(jnp.bfloat16)
        x_ref[at, feat:] = (far_buf[at, :] * (1.0 / fan_two)).astype(jnp.bfloat16)
    x_ref[hops:, :feat] = own_buf[hops:, :].astype(jnp.bfloat16)
    x_ref[hops:, feat:] = (row_sum * (1.0 / fan_one)).astype(jnp.bfloat16)


def front_kernel(
    hop2_hbm, hop1_hbm, seed_hbm, map_hbm, feat_hbm,
    table_ref, addr_ref,
    hop2_ref, hop1_ref, seed_ref, ids_ref, pos_ref, own_ref, val_ref, slot_ref, map_ref, feat_ref, wide, stage_a, stage_b, row_stage,
    req_ref, inbox, send, ids_smem, wanted,
    local_sem, req_send, req_recv, hub_send, hub_recv, row_send, row_recv, *, parts, shift, cap_row,
):
    node_rows = feat_ref.shape[0]
    me = lax.axis_index("dom")
    core, z, x = lax.rem(me, 2), lax.rem(me // 2, N_Z), me // (2 * N_Z)
    barrier = pltpu.get_barrier_semaphore()

    get_ids = [
        pltpu.make_async_copy(source, target, local_sem.at[6 + n])
        for n, (source, target) in enumerate(((hop2_hbm, hop2_ref), (hop1_hbm, hop1_ref), (seed_hbm, seed_ref)))
    ]
    for each in get_ids:
        each.start()
    get_map = pltpu.make_async_copy(map_hbm, map_ref, local_sem.at[0])
    get_map.start()
    get_feat = pltpu.make_async_copy(feat_hbm, feat_ref, local_sem.at[1])
    get_feat.start()
    x_rows = N_Z * HOT_DEV
    half = N_X * x_rows
    own_at = pl.ds(pl.multiple_of(core * half + (x * N_Z + z) * HOT_DEV, HOT_DEV), HOT_DEV)
    keep_hub = pltpu.make_async_copy(feat_hbm.at[pl.ds(0, HOT_DEV)], table_ref.at[own_at], local_sem.at[2])
    keep_hub.start()

    def peer(step):
        k = lax.rem(step, 8)
        dz = lax.rem(N_Z + 4 + (lax.rem(k, 2) * 2 - 1) * ((k + 1) // 2), N_Z)
        dxc = lax.rem(step // 8 + 1, 8)
        other = (lax.rem(x + dxc // 2, N_X) * N_Z + lax.rem(z + dz, N_Z)) * 2 + lax.rem(core + lax.rem(dxc, 2), 2)
        return other, {"dom": other}

    def greet(step, carry):
        pl.semaphore_signal(barrier, inc=1, device_id=peer(step)[1], device_id_type=MESH)
        return carry

    lax.fori_loop(0, parts - 1, greet, 0)

    for each in get_ids:
        each.wait()
    place_ids(hop2_ref, hop1_ref, seed_ref, ids_ref)
    slot_ref[...] = ids_ref[...] >> 7
    ids_down = pltpu.make_async_copy(slot_ref, ids_smem, local_sem.at[3])
    ids_down.start()
    get_feat.wait()

    def widen(step, carry):
        at = pl.ds(pl.multiple_of(step * 64, 64), 64)
        wide[at, :] = feat_ref[at, :].astype(jnp.float32)
        return carry

    lax.fori_loop(0, node_rows // 64, widen, 0)
    keep_hub.wait()

    def hub_copy(at, level, where):
        return pltpu.make_async_remote_copy(
            table_ref.at[at], table_ref.at[at], hub_send.at[level], hub_recv.at[level],
            device_id=where, device_id_type=MESH,
        )

    def hub_wait(rows, level):
        return hub_copy(pl.ds(0, rows), level, peer(0)[1])

    def send_z(step, carry):
        hub_copy(own_at, 0, {"dom": (x * N_Z + lax.rem(z + step, N_Z)) * 2 + core}).start()
        return carry

    def x_at(step):
        return pl.ds(pl.multiple_of(core * half + lax.rem(x + step, N_X) * x_rows, x_rows), x_rows)

    def send_x(first, rows):
        at = pl.ds(pl.multiple_of(core * half + x * x_rows + first, 8), rows)

        def one(step, carry):
            hub_copy(at, 1, {"dom": (lax.rem(x + step, N_X) * N_Z + z) * 2 + core}).start()
            return carry

        lax.fori_loop(1, N_X, one, 0)

    def send_core(step, carry):
        hub_copy(x_at(step), 2, {"dom": me + 1 - 2 * core}).start()
        return carry

    get_map.wait()
    ids_down.wait()

    def lookup(step, carry):
        lookup_step(step, ids_ref, ids_smem, map_ref, stage_a, stage_b, pos_ref)
        return carry

    groups = -(-ID_ROWS // 4)
    lax.fori_loop(0, groups // 3, lookup, 0)
    pl.semaphore_wait(barrier, parts - 1)
    lax.fori_loop(1, N_Z, send_z, 0)
    lax.fori_loop(groups // 3, groups, lookup, 0)
    for r in range(groups * 4, pos_ref.shape[0]):
        pos_ref[r : r + 1, :] = jnp.zeros((1, LANES), jnp.int32)
    assign(
        pos_ref, own_ref, val_ref, slot_ref, addr_ref, req_ref, parts=parts, shift=shift, cap_row=cap_row,
    )
    ask_at = pl.ds(0, 1)
    keep_req = pltpu.make_async_copy(req_ref.at[me], inbox.at[me], local_sem.at[4])
    keep_req.start()

    def ask(step, carry):
        other, where = peer(step)
        pltpu.make_async_remote_copy(
            req_ref.at[other, ask_at], inbox.at[me, ask_at], req_send, req_recv, device_id=where, device_id_type=MESH
        ).start()
        return carry

    lax.fori_loop(0, parts - 1, ask, 0)
    hub_wait((N_Z - 1) * HOT_DEV, 0).wait_recv()
    x_early = x_rows // 4
    x_each = (x_rows - x_early) // parts
    send_x(0, x_early)
    lax.fori_loop(0, 1, send_core, 0)
    most = pl.ds(0, parts - 1)
    asked = pltpu.make_async_remote_copy(
        req_ref.at[most, ask_at], inbox.at[most, ask_at], req_send, req_recv,
        device_id=peer(0)[1], device_id_type=MESH,
    )
    keep_req.wait()
    asked.wait_recv()
    to_scalar = pltpu.make_async_copy(inbox.at[:, ask_at], wanted, local_sem.at[5])
    to_scalar.start()
    to_scalar.wait()

    def collect(other):
        asked_rows = wanted.at[other, 0]
        for i in range(cap_row):
            row_stage[i : i + 1, :] = wide[pl.ds(asked_rows[i], 1), :]
        return row_stage[...].astype(jnp.bfloat16)

    def rows_at(part):
        return pl.ds(pl.multiple_of(HUB_ROWS + part * cap_row, 8), cap_row)

    def serve(step, carry):
        other, where = peer(step)
        send[other] = collect(other)
        pltpu.make_async_remote_copy(
            send.at[other], table_ref.at[rows_at(me)], row_send, row_recv, device_id=where, device_id_type=MESH
        ).start()
        send_x(x_early + step * x_each, x_each)
        return carry

    lax.fori_loop(0, parts - 1, serve, 0)
    send_x(x_early + (parts - 1) * x_each, x_each)
    table_ref[rows_at(me), :] = collect(me)
    hub_wait((N_X - 1) * x_rows, 1).wait_recv()
    lax.fori_loop(1, N_X, send_core, 0)

    asked.wait_send()
    hub_wait((N_Z - 1) * HOT_DEV, 0).wait_send()
    hub_wait((N_X - 1) * x_rows, 1).wait_send()
    hub_wait(half, 2).wait()
    pltpu.make_async_remote_copy(
        send.at[most], send.at[most], row_send, row_recv, device_id=peer(0)[1], device_id_type=MESH
    ).wait()


def front(hop2, hop1, seed_ids, partition_map, features, cap_row):
    parts = lax.axis_size("dom")
    node_rows, feat = features.shape
    vmem = pl.BlockSpec(memory_space=pltpu.VMEM)
    hbm = pl.BlockSpec(memory_space=pltpu.HBM)
    rows = round_up(ID_ROWS, 8)
    table_rows = HUB_ROWS + parts * cap_row
    return pl.pallas_call(
        functools.partial(front_kernel, parts=parts, shift=node_rows.bit_length() - 1, cap_row=cap_row),
        name="front",
        out_shape=(
            jax.ShapeDtypeStruct((table_rows, feat), features.dtype),
            jax.ShapeDtypeStruct((rows, LANES), jnp.int32),
        ),
        in_specs=[hbm] * 5,
        out_specs=(vmem, vmem),
        scratch_shapes=[
            pltpu.VMEM(hop2.shape, jnp.int32),
            pltpu.VMEM(hop1.shape, jnp.int32),
            pltpu.VMEM((1, seed_ids.size), jnp.int32),
        ]
        + [pltpu.VMEM((rows, LANES), jnp.int32)] * 5
        + [
            pltpu.VMEM((partition_map.size // LANES, LANES), jnp.int32),
            pltpu.VMEM((node_rows, feat), features.dtype),
            pltpu.VMEM((node_rows, feat), jnp.float32),
            pltpu.VMEM((2 * LANES, LANES), jnp.int32),
            pltpu.VMEM((2 * LANES, LANES), jnp.int32),
            pltpu.VMEM((cap_row, feat), jnp.float32),
            pltpu.VMEM((parts, 8, LANES), jnp.int32),
            pltpu.VMEM((parts, 8, LANES), jnp.int32),
            pltpu.VMEM((parts, cap_row, feat), features.dtype),
            pltpu.SMEM((rows, LANES), jnp.int32),
            pltpu.SMEM((parts, 1, LANES), jnp.int32),
            pltpu.SemaphoreType.DMA((9,)),
            pltpu.SemaphoreType.DMA,
            pltpu.SemaphoreType.DMA,
            pltpu.SemaphoreType.DMA((3,)),
            pltpu.SemaphoreType.DMA((3,)),
            pltpu.SemaphoreType.DMA,
            pltpu.SemaphoreType.DMA,
        ],
        compiler_params=pltpu.CompilerParams(collective_id=2, has_side_effects=True, vmem_limit_bytes=24 * MIB),
    )(
        *(
            pltpu.with_memory_space_constraint(each, pltpu.HBM)
            for each in (hop2, hop1, seed_ids.reshape(1, -1), partition_map.reshape(-1, LANES), features)
        )
    )

def fetch_kernel(addr_smem, table_ref, x_ref, table_wide, own_buf, far_buf, *, seeds, fan_one, fan_two):
    def widen(step, carry):
        at = pl.ds(pl.multiple_of(step * 128, 128), 128)
        table_wide[at, :] = table_ref[at, :].astype(jnp.float32)
        return carry

    lax.fori_loop(0, table_ref.shape[0] // 128, widen, 0)
    fetch_rows(addr_smem, table_wide, own_buf, far_buf, x_ref, seeds=seeds, fan_one=fan_one, fan_two=fan_two)


def fetch_all(addr, table, seeds, fan_one, fan_two):
    feat = table.shape[1]
    total = seeds * (1 + fan_one)
    vmem = pl.BlockSpec(memory_space=pltpu.VMEM)
    return pl.pallas_call(
        functools.partial(fetch_kernel, seeds=seeds, fan_one=fan_one, fan_two=fan_two),
        name="fetch",
        out_shape=jax.ShapeDtypeStruct((total, 2 * feat), table.dtype),
        in_specs=[pl.BlockSpec(memory_space=pltpu.SMEM), vmem],
        out_specs=vmem,
        scratch_shapes=[
            pltpu.VMEM(table.shape, jnp.float32),
            pltpu.VMEM((total, feat), jnp.float32),
            pltpu.VMEM((total, feat), jnp.float32),
        ],
        compiler_params=pltpu.CompilerParams(vmem_limit_bytes=24 * MIB),
    )(addr, table)


ROOT = 0.7978845608028654
CUBE = 0.044715


def gelu_pair(pre):
    square = pre * pre
    bend = jnp.tanh(ROOT * pre * (1.0 + CUBE * square))
    half = 0.5 * (1.0 + bend)
    slope = half + 0.5 * pre * (1.0 - bend * bend) * (ROOT * (1.0 + 3.0 * CUBE * square))
    return pre * half, slope


N_REP = 4
MEMBERS = N_X * N_REP * 2
PART_TWO = 24
PART_ONE = 16
PART = PART_TWO + PART_ONE
HIGH = 176


def pack_two(part_ref, g_two, gb_two):
    classes, width = g_two.shape
    for h in range(width // LANES):
        for b in range(HIGH // 8):
            block = h * (HIGH // 8) + b
            to = block % 3 * 8
            rows = min(8, classes - b * 8)
            part_ref[block // 3, to : to + rows, :] = g_two[
                b * 8 : b * 8 + rows, h * LANES : (h + 1) * LANES
            ].astype(jnp.bfloat16)
            if rows < 8:
                part_ref[block // 3, to + rows : to + 8, :] = jnp.zeros((8 - rows, LANES), jnp.bfloat16)
    first = width // LANES * (HIGH // 8)
    for block in range(first, MEMBERS * 3):
        to = block % 3 * 8
        part_ref[block // 3, to : to + 8, :] = jnp.zeros((8, LANES), jnp.bfloat16)
    to = first % 3 * 8
    part_ref[first // 3, to : to + 1, :] = gb_two[:, :LANES].astype(jnp.bfloat16)
    part_ref[first // 3, to + 1 : to + 2, : classes - LANES] = gb_two[:, LANES:].astype(jnp.bfloat16)


def pack_one(part_ref, g_one, gb_one):
    halves = g_one.shape[1] // LANES
    each = g_one.shape[0] // PART_ONE
    for h in range(halves):
        for i in range(each):
            part_ref[h * each + i, PART_TWO:, :] = g_one[
                i * PART_ONE : (i + 1) * PART_ONE, h * LANES : (h + 1) * LANES
            ].astype(jnp.bfloat16)
        part_ref[MEMBERS - 1, 16 + h : 17 + h, :] = gb_one[:, h * LANES : (h + 1) * LANES].astype(jnp.bfloat16)


def dense_kernel(
    x_ref, label_ref, self_one, neigh_one, b_one_ref, self_two, neigh_two, b_two_ref,
    loss_ref, gathered,
    slope_buf, d_buf, part_ref, box, z_box, send_sem, recv_sem, *, seeds, fan_one,
):
    hidden = self_one.shape[1]
    hops = seeds * fan_one
    me, y = lax.axis_index("dom"), lax.axis_index("rep")
    core, z, x = lax.rem(me, 2), lax.rem(me // 2, N_Z), me // (2 * N_Z)
    mine = (x * N_REP + y) * 2 + core
    barrier = pltpu.get_barrier_semaphore()

    def spread(k, size):
        return lax.rem(size + size // 2 + (lax.rem(k, 2) * 2 - 1) * ((k + 1) // 2), size)

    def near(step):
        other_x = lax.rem(x + spread(step // 8, N_X), N_X)
        other_y = lax.rem(y + spread(lax.rem(step // 2, N_REP), N_REP), N_REP)
        other_core = lax.rem(core + lax.rem(step + 1, 2), 2)
        where = {"dom": (other_x * N_Z + z) * 2 + other_core, "rep": other_y}
        return (other_x * N_REP + other_y) * 2 + other_core, where

    def far(step):
        return {"dom": (x * N_Z + lax.rem(z + spread(step, N_Z), N_Z)) * 2 + core, "rep": y}

    def greet_near(step, carry):
        pl.semaphore_signal(barrier, inc=1, device_id=near(step)[1], device_id_type=MESH)
        return carry

    def greet_far(step, carry):
        pl.semaphore_signal(barrier, inc=1, device_id=far(step), device_id_type=MESH)
        return carry

    lax.fori_loop(0, N_Z - 1, greet_far, 0)
    lax.fori_loop(0, MEMBERS - 1, greet_near, 0)

    w_one = jnp.concatenate([self_one[...], neigh_one[...]], axis=0)
    w_two = jnp.concatenate([self_two[...], neigh_two[...]], axis=1)
    b_one = b_one_ref[...]
    hid_sum = jnp.zeros((seeds, hidden), jnp.float32)
    act = None
    for j in range(fan_one + 1):
        at = slice(j * seeds, (j + 1) * seeds)
        act, slope = gelu_pair(dot_nn(x_ref[at, :], w_one) + b_one)
        act = act.astype(jnp.bfloat16)
        slope_buf[at, :] = slope
        if j < fan_one:
            hid_sum = hid_sum + act.astype(jnp.float32)
    hid = jnp.concatenate([act, (hid_sum * (1.0 / fan_one)).astype(jnp.bfloat16)], axis=1)
    logits = dot_nt(hid, w_two) + b_two_ref[...]
    shifted = logits - jnp.max(logits, axis=1, keepdims=True)
    log_probs = shifted - jnp.log(jnp.sum(jnp.exp(shifted), axis=1, keepdims=True))
    class_iota = lax.broadcasted_iota(jnp.int32, logits.shape, 1)
    diagonal = lax.broadcasted_iota(jnp.int32, (seeds, seeds), 0) == lax.broadcasted_iota(jnp.int32, (seeds, seeds), 1)
    label = jnp.sum(jnp.where(diagonal, label_ref[...].astype(jnp.float32), 0.0), axis=1, keepdims=True)
    target = (class_iota.astype(jnp.float32) == label).astype(jnp.float32)
    loss = jnp.sum(log_probs * target, axis=1, keepdims=True)
    loss_ref[...] = -jnp.sum(jnp.where(diagonal, loss, 0.0), axis=0, keepdims=True)
    d_logits = ((jnp.exp(log_probs) - target) * (1.0 / seeds)).astype(jnp.bfloat16)
    pack_two(part_ref, dot_tn(d_logits, hid), jnp.sum(d_logits.astype(jnp.float32), axis=0, keepdims=True))
    pl.semaphore_wait(barrier, MEMBERS + N_Z - 2)

    def copy(source, target, stage, where):
        return pltpu.make_async_remote_copy(
            source, target, send_sem.at[stage], recv_sem.at[stage], device_id=where, device_id_type=MESH
        )

    two_at, one_at = pl.ds(0, PART_TWO), pl.ds(PART_TWO, PART_ONE)

    def send_two(step, carry):
        other, where = near(step)

        @pl.when(other < MEMBERS - 1)
        def _():
            copy(part_ref.at[other, two_at], box.at[mine, two_at], 0, where).start()

        return carry

    lax.fori_loop(0, MEMBERS - 1, send_two, 0)
    d_hid = dot_nn(d_logits, w_two)
    d_hop = d_hid[:, hidden:] * (1.0 / fan_one)
    for j in range(fan_one + 1):
        at = slice(j * seeds, (j + 1) * seeds)
        d_pre = ((d_hop if j < fan_one else d_hid[:, :hidden]) * slope_buf[at, :]).astype(jnp.bfloat16)
        d_buf[at, :] = d_pre
    gb_one = dot_nn(jnp.ones((8, d_buf.shape[0]), jnp.bfloat16), d_buf[...])[:1]
    pack_one(part_ref, dot_tn(x_ref[...], d_buf[...]), gb_one)

    def send_one(step, carry):
        other, where = near(step)
        copy(part_ref.at[other, one_at], box.at[mine, one_at], 0, where).start()

        @pl.when(other == MEMBERS - 1)
        def _():
            copy(part_ref.at[other, two_at], box.at[mine, two_at], 0, where).start()

        return carry

    lax.fori_loop(0, MEMBERS - 1, send_one, 0)
    box[mine] = part_ref[mine]
    some = box.at[pl.ds(0, MEMBERS - 1)]
    first = copy(some, some, 0, near(0)[1])
    first.wait_recv()
    total = box[0].astype(jnp.float32)
    for i in range(1, MEMBERS):
        total = total + box[i].astype(jnp.float32)
    z_box[z] = total

    def across(step, carry):
        copy(z_box.at[z], z_box.at[z], 1, far(step)).start()
        return carry

    lax.fori_loop(0, N_Z - 1, across, 0)
    some = z_box.at[pl.ds(0, N_Z - 1)]
    second = copy(some, some, 1, far(0))
    second.wait_recv()
    total = z_box[0]
    for i in range(1, N_Z):
        total = total + z_box[i]
    gathered[mine] = total.astype(jnp.bfloat16)

    def back(step, carry):
        copy(gathered.at[mine], gathered.at[mine], 2, near(step)[1]).start()
        return carry

    lax.fori_loop(0, MEMBERS - 1, back, 0)
    some = gathered.at[pl.ds(0, MEMBERS - 1)]
    third = copy(some, some, 2, near(0)[1])
    third.wait_recv()
    first.wait_send()
    second.wait_send()
    third.wait_send()


def dense(x, labels, self_one, neigh_one, bias_one, self_two, neigh_two, bias_two, fan_one):
    seeds = labels.shape[0]
    hidden = self_one.shape[1]
    classes = self_two.shape[1]
    total = x.shape[0]
    vmem = pl.BlockSpec(memory_space=pltpu.VMEM)
    return pl.pallas_call(
        functools.partial(dense_kernel, seeds=seeds, fan_one=fan_one),
        name="dense",
        out_shape=(
            jax.ShapeDtypeStruct((1, seeds), jnp.float32),
            jax.ShapeDtypeStruct((MEMBERS, PART, LANES), jnp.bfloat16),
        ),
        in_specs=[vmem] * 8,
        out_specs=(vmem,) * 2,
        scratch_shapes=[
            pltpu.VMEM((total, hidden), jnp.float32),
            pltpu.VMEM((total, hidden), jnp.bfloat16),
            pltpu.VMEM((MEMBERS, PART, LANES), jnp.bfloat16),
            pltpu.VMEM((MEMBERS, PART, LANES), jnp.bfloat16),
            pltpu.VMEM((N_Z, PART, LANES), jnp.float32),
            pltpu.SemaphoreType.DMA((3,)),
            pltpu.SemaphoreType.DMA((3,)),
        ],
        compiler_params=pltpu.CompilerParams(collective_id=1, has_side_effects=True, vmem_limit_bytes=16 * MIB),
    )(
        x,
        labels.reshape(1, seeds),
        self_one,
        neigh_one,
        bias_one.reshape(1, hidden),
        self_two.T,
        neigh_two.T,
        bias_two.reshape(1, classes),
    )


def unpack_kernel(gathered, loss_in, loss_out, self_one, neigh_one, bias_one, self_two, neigh_two, bias_two):
    feat, hidden = self_one.shape
    classes = self_two.shape[0]
    loss_out[...] = loss_in[...]
    halves = hidden // LANES
    each = feat // PART_ONE
    for h in range(halves):
        cols = slice(h * LANES, (h + 1) * LANES)
        for i in range(each):
            at = slice(i * PART_ONE, (i + 1) * PART_ONE)
            self_one[at, cols] = gathered[h * 2 * each + i, PART_TWO:, :].astype(jnp.float32)
            neigh_one[at, cols] = gathered[h * 2 * each + each + i, PART_TWO:, :].astype(jnp.float32)
        for b in range(HIGH // 8):
            rows = min(8, classes - b * 8)
            for k, out in enumerate((self_two, neigh_two)):
                block = (k * halves + h) * (HIGH // 8) + b
                to = block % 3 * 8
                out[b * 8 : b * 8 + rows, cols] = gathered[block // 3, to : to + 8, :].astype(jnp.float32)[:rows]
        bias_one[:, cols] = gathered[MEMBERS - 1, 16:24, :].astype(jnp.float32)[h : h + 1]
    first = 2 * halves * (HIGH // 8)
    to = first % 3 * 8
    last = gathered[first // 3, to : to + 8, :].astype(jnp.float32)
    bias_two[:, :LANES] = last[:1]
    bias_two[:, LANES:] = last[1:2, : classes - LANES]


def unpack(gathered, loss, feat, hidden, classes):
    vmem = pl.BlockSpec(memory_space=pltpu.VMEM)
    shapes = [loss.shape, (feat, hidden), (feat, hidden), (1, hidden), (classes, hidden), (classes, hidden), (1, classes)]
    return pl.pallas_call(
        unpack_kernel,
        name="unpack",
        out_shape=tuple(jax.ShapeDtypeStruct(shape, jnp.float32) for shape in shapes),
        in_specs=[vmem] * 2,
        out_specs=(vmem,) * 7,
        compiler_params=pltpu.CompilerParams(vmem_limit_bytes=8 * MIB),
    )(gathered, loss)


def shards(
    features, partition_map, seed_ids, hop1_ids, hop2_ids, labels,
    self_one, neigh_one, bias_one, self_two, neigh_two, bias_two,
):
    parts = lax.axis_size("dom")
    seeds = seed_ids.shape[0]
    fan_one = hop1_ids.shape[1]
    fan_two = hop2_ids.shape[2]
    feat = features.shape[1]
    tree_rows = 1 + fan_one + fan_one * fan_two
    cold_cap = tree_rows // 2 * (seeds // parts)
    cap_row = round_up(cold_cap, 8)
    table, addr = front(hop2_ids.transpose(2, 1, 0), hop1_ids.T, seed_ids, partition_map, features, cap_row)
    x = fetch_all(addr, table, seeds, fan_one, fan_two)
    hidden, classes = self_two.shape
    loss, gathered = dense(x, labels, self_one, neigh_one, bias_one, self_two, neigh_two, bias_two, fan_one)
    loss, *grads = unpack(gathered, loss, feat, hidden, classes)
    return (
        loss.reshape(-1), grads[0], grads[1], grads[2].reshape(-1),
        grads[3].T, grads[4].T, grads[5].reshape(-1),
    )


def solution(mesh):
    return jax.shard_map(
        shards,
        mesh=mesh,
        in_specs=(
            P("dom", None),
            P(),
            P(("dom", "rep")),
            P(("dom", "rep"), None),
            P(("dom", "rep"), None, None),
            P(("dom", "rep")),
            P(),
            P(),
            P(),
            P(),
            P(),
            P(),
        ),
        out_specs=(P(("dom", "rep")), P(), P(), P(), P(), P(), P()),
        check_vma=False,
    )
```

```python
import functools

import jax
import jax.numpy as jnp
from jax import lax
from jax.experimental import pallas as pl
from jax.experimental.pallas import tpu as pltpu
from jax.sharding import PartitionSpec as P

HOT_DEV = 256
LANES = 128
MESH = pl.DeviceIdType.MESH
MIB = 1024 * 1024


def round_up(value, unit):
    return -(-value // unit) * unit


def dot_tn(left, right):
    return lax.dot_general(left, right, (((0,), (0,)), ((), ())), preferred_element_type=jnp.float32)


def dot_nt(left, right):
    return lax.dot_general(left, right, (((1,), (1,)), ((), ())), preferred_element_type=jnp.float32)


def dot_nn(left, right):
    return jnp.dot(left, right, preferred_element_type=jnp.float32)


N_X, N_Z = 4, 8
ID_ROWS = 83
HUB_ROWS = 64 * HOT_DEV


def place_ids(hop2_ref, hop1_ref, seed_ref, ids_ref):
    fan_two, fan_one, seeds = hop2_ref.shape
    half = fan_two // 2
    ids_ref[...] = jnp.zeros(ids_ref.shape, jnp.int32)
    for m in range(half):
        at = slice(m * fan_one, (m + 1) * fan_one)
        ids_ref[at, :seeds] = hop2_ref[m]
        ids_ref[at, seeds:] = hop2_ref[half + m]
    top = half * fan_one
    ids_ref[top : top + 8, :seeds] = hop1_ref[:8, :]
    ids_ref[top : top + fan_one - 8, seeds:] = hop1_ref[8:, :]
    ids_ref[top + fan_one - 8 : top + fan_one - 7, seeds:] = seed_ref[...]


def gather_map(first, smem_ref, map_ref, stage):
    for r in range(stage.shape[0] // LANES):
        high = smem_ref.at[first + r]
        for i in range(LANES):
            stage[r * LANES + i : r * LANES + i + 1, :] = map_ref[pl.ds(high[i], 1), :]


def pick_lanes(first, ids_ref, stage, pos_ref):
    sub_iota = lax.broadcasted_iota(jnp.int32, (LANES, LANES), 0)
    lane_iota = lax.broadcasted_iota(jnp.int32, (LANES, LANES), 1)
    for r in range(stage.shape[0] // LANES):
        got = stage[r * LANES : (r + 1) * LANES, :]
        pieces = jnp.concatenate([got >> 16, (got >> 8) & 255, got & 255], axis=0)
        pieces = pieces.astype(jnp.float32).astype(jnp.bfloat16)
        low = ids_ref[pl.ds(first + r, 1), :] & (LANES - 1)
        hot = (sub_iota == low).astype(jnp.float32).astype(jnp.bfloat16)
        found = dot_nn(pieces, hot)
        found = found[:LANES] * 65536.0 + found[LANES : 2 * LANES] * 256.0 + found[2 * LANES :]
        picked = jnp.sum(jnp.where(sub_iota == lane_iota, found, 0.0), axis=0, keepdims=True)
        pos_ref[pl.ds(first + r, 1), :] = picked.astype(jnp.int32)


def lookup_step(step, ids_ref, smem_ref, map_ref, stage_a, stage_b, pos_ref):
    first = step * 4
    gather_map(first, smem_ref, map_ref, stage_a)

    pick_lanes(first, ids_ref, stage_a, pos_ref)
    gather_map(first + 2, smem_ref, map_ref, stage_b)
    pick_lanes(first + 2, ids_ref, stage_b, pos_ref)


def assign(pos_ref, own_ref, val_ref, slot_ref, addr_ref, req_ref, *, parts, shift, cap_row):
    rows = pos_ref.shape[0]
    position = pos_ref[...]
    owner = position >> shift
    local = position & ((1 << shift) - 1)
    row_iota = lax.broadcasted_iota(jnp.int32, (rows, LANES), 0)
    is_cold = (local >= HOT_DEV) & (row_iota < ID_ROWS)
    own_ref[...] = jnp.where(is_cold, owner, -1)
    val_ref[...] = local
    part_iota = lax.broadcasted_iota(jnp.int32, (parts, LANES), 0)
    slot_iota = lax.broadcasted_iota(jnp.int32, (LANES, LANES), 0)
    upper = lax.broadcasted_iota(jnp.int32, (LANES, 2 * LANES), 0) <= lax.broadcasted_iota(
        jnp.int32, (LANES, 2 * LANES), 1
    )
    upper = upper.astype(jnp.float32).astype(jnp.bfloat16)

    def block(step, carry):
        base, table = carry
        at = pl.ds(pl.multiple_of(step * 8, 8), 8)
        own8 = own_ref[at, :]
        val8 = val_ref[at, :].astype(jnp.float32)
        top8 = jnp.floor(val8 * (1.0 / LANES))
        low8 = val8 - top8 * LANES
        slots, lefts = [], []
        for q in range(8):
            mine = part_iota == own8[q : q + 1, :]
            counts = dot_nn(mine.astype(jnp.float32).astype(jnp.bfloat16), upper)
            slots.append(jnp.sum(jnp.where(mine, counts[:, :LANES] + base, 0.0), axis=0, keepdims=True) - 1.0)
            base = base + counts[:, LANES:]
            lefts.append(
                jnp.concatenate(
                    [jnp.where(mine, top8[q : q + 1, :], 0.0), jnp.where(mine, low8[q : q + 1, :], 0.0)], axis=0
                ).astype(jnp.bfloat16)
            )
        slot8 = jnp.concatenate(slots, axis=0).astype(jnp.int32)
        slot_ref[at, :] = slot8
        for q in range(0, 8, 2):
            rights = [
                (slot_iota == slot8[k : k + 1, :]).astype(jnp.float32).astype(jnp.bfloat16) for k in (q, q + 1)
            ]
            table = table + dot_nt(
                jnp.concatenate([lefts[q], lefts[q + 1]], axis=1), jnp.concatenate(rights, axis=1)
            )
        return base, table

    start = (jnp.zeros((parts, LANES), jnp.float32), jnp.zeros((2 * parts, LANES), jnp.float32))
    table = lax.fori_loop(0, rows // 8, block, start)[1]
    request = (table[:parts] * LANES + table[parts:]).astype(jnp.int32) & ((1 << shift) - 1)
    for p in range(parts):
        req_ref[p, 0:1, :] = request[p : p + 1, :]
    hot_addr = (owner & 1) * (HUB_ROWS // 2) + (owner >> 1) * HOT_DEV + (local & (HOT_DEV - 1))
    addr = jnp.where(is_cold, HUB_ROWS + owner * cap_row + slot_ref[...], hot_addr)
    addr_ref[...] = jnp.clip(addr, 0, HUB_ROWS + parts * cap_row - 1)


def tree_sum(values):
    while len(values) > 1:
        values = [a + b for a, b in zip(values[::2], values[1::2])] + (
            [values[-1]] if len(values) % 2 else []
        )
    return values[0]


def fetch_rows(addr_smem, wide, own_buf, far_buf, x_ref, *, seeds, fan_one, fan_two):
    hops = seeds * fan_one
    feat = wide.shape[1]
    half = fan_two // 2
    top = half * fan_one

    def fetch(j, carry):
        late = j // 8
        own_at = addr_smem.at[top + j - 8 * late, pl.ds(pl.multiple_of(late * seeds, seeds), seeds)]
        far_at = [addr_smem.at[m * fan_one + j] for m in range(half)]
        base = pl.multiple_of(j * seeds, seeds)
        own_out, far_out = own_buf.at[pl.ds(base, seeds)], far_buf.at[pl.ds(base, seeds)]
        for k in range(seeds):
            own_out[k : k + 1, :] = wide[pl.ds(own_at[k], 1), :]
            rows = [wide[pl.ds(far_at[m % half][m // half * seeds + k], 1), :] for m in range(fan_two)]
            far_out[k : k + 1, :] = tree_sum(rows)
        return carry

    lax.fori_loop(0, fan_one, fetch, 0)

    def fetch_seed(step, carry):
        base = pl.multiple_of(step * 8, 8)
        for k in range(8):
            own_buf[pl.ds(hops + base + k, 1), :] = wide[
                pl.ds(addr_smem[top + fan_one - 8, seeds + base + k], 1), :
            ]
        return carry

    lax.fori_loop(0, seeds // 8, fetch_seed, 0)
    row_sum = jnp.zeros((seeds, feat), jnp.float32)
    for j in range(fan_one):
        at = slice(j * seeds, (j + 1) * seeds)
        own = own_buf[at, :]
        row_sum = row_sum + own
        x_ref[at, :feat] = own.astype(jnp.bfloat16)
        x_ref[at, feat:] = (far_buf[at, :] * (1.0 / fan_two)).astype(jnp.bfloat16)
    x_ref[hops:, :feat] = own_buf[hops:, :].astype(jnp.bfloat16)
    x_ref[hops:, feat:] = (row_sum * (1.0 / fan_one)).astype(jnp.bfloat16)


def front_kernel(
    hop2_hbm, hop1_hbm, seed_hbm, map_hbm, feat_hbm,
    table_ref, addr_ref,
    hop2_ref, hop1_ref, seed_ref, ids_ref, pos_ref, own_ref, val_ref, slot_ref, map_ref, feat_ref, wide, stage_a, stage_b, row_stage,
    req_ref, inbox, send, ids_smem, wanted,
    local_sem, scalar_sem, req_send, req_recv, hub_send, hub_recv, row_send, row_recv, *, parts, shift, cap_row,
):
    node_rows = feat_ref.shape[0]
    me = lax.axis_index("dom")
    core, z, x = me & 1, (me >> 1) & (N_Z - 1), me >> 4
    barrier = pltpu.get_barrier_semaphore()

    get_ids = [
        pltpu.make_async_copy(source, target, local_sem.at[6 + n])
        for n, (source, target) in enumerate(((hop2_hbm, hop2_ref), (hop1_hbm, hop1_ref), (seed_hbm, seed_ref)))
    ]
    for each in get_ids:
        each.start()
    get_map = pltpu.make_async_copy(map_hbm, map_ref, local_sem.at[0])
    get_map.start()
    get_feat = pltpu.make_async_copy(feat_hbm, feat_ref, local_sem.at[1])
    get_feat.start()
    x_rows = N_Z * HOT_DEV
    half = N_X * x_rows
    own_at = pl.ds(pl.multiple_of(core * half + (x * N_Z + z) * HOT_DEV, HOT_DEV), HOT_DEV)
    keep_hub = pltpu.make_async_copy(feat_hbm.at[pl.ds(0, HOT_DEV)], table_ref.at[own_at], local_sem.at[2])
    keep_hub.start()

    def turn_of(kind):
        return ((kind >> 1) + 1) * (1 - 2 * (kind & 1))

    def peer(dz, r, sign):
        other = (((x + sign * (r >> 1)) & (N_X - 1)) << 4) + (((z + sign * dz) & (N_Z - 1)) << 1) + (core ^ (r & 1))
        return other, {"dom": other}

    def all_peers(act):
        def kind(k, carry):
            def one(r, inner):
                act(k, k * 8 + r, *peer(turn_of(k), r, 1))
                return inner

            lax.fori_loop(0, 8, one, 0)
            return carry

        lax.fori_loop(0, N_Z - 1, kind, 0)

        def flat(r, carry):
            act(N_Z - 1, (N_Z - 1) * 8 + r - 1, *peer(0, r, 1))
            return carry

        lax.fori_loop(1, 8, flat, 0)

    def greet(k, slot, other, where):
        pl.semaphore_signal(barrier, inc=1, device_id=where, device_id_type=MESH)

    all_peers(greet)

    for each in get_ids:
        each.wait()
    place_ids(hop2_ref, hop1_ref, seed_ref, ids_ref)
    slot_ref[...] = ids_ref[...] >> 7
    ids_down = pltpu.make_async_copy(slot_ref, ids_smem, local_sem.at[3])
    ids_down.start()
    get_feat.wait()

    def widen(step, carry):
        at = pl.ds(pl.multiple_of(step * 64, 64), 64)
        wide[at, :] = feat_ref[at, :].astype(jnp.float32)
        return carry

    lax.fori_loop(0, node_rows // 64, widen, 0)
    keep_hub.wait()

    def hub_copy(at, level, where):
        return pltpu.make_async_remote_copy(
            table_ref.at[at], table_ref.at[at], hub_send.at[level], hub_recv.at[level],
            device_id=where, device_id_type=MESH,
        )

    def hub_wait(rows, level):
        return hub_copy(pl.ds(0, rows), level, peer(1, 0, 1)[1])

    x_each = 72
    x_early = x_rows - (parts - 1) // (N_X - 1) * x_each

    def send_z(step, carry):
        hub_copy(own_at, 0, peer(step, 0, 1)[1]).start()
        return carry

    def x_at(step):
        return pl.ds(pl.multiple_of(core * half + ((x + step) & (N_X - 1)) * x_rows, x_rows), x_rows)

    def send_x(first, rows):
        at = pl.ds(pl.multiple_of(core * half + x * x_rows + first, 8), rows)

        def one(step, carry):
            hub_copy(at, 1, peer(0, 2 * step, 1)[1]).start()
            return carry

        lax.fori_loop(1, N_X, one, 0)

    def send_x_one(step):
        turn = step // (N_X - 1)
        first = x_early + turn * x_each
        at = pl.ds(pl.multiple_of(core * half + x * x_rows + first, 8), x_each)
        hub_copy(at, 1, peer(0, 2 * (step - turn * (N_X - 1) + 1), 1)[1]).start()

    def send_core(step, carry):
        hub_copy(x_at(step), 2, {"dom": me + 1 - 2 * core}).start()
        return carry

    get_map.wait()
    ids_down.wait()

    def lookup(step, carry):
        lookup_step(step, ids_ref, ids_smem, map_ref, stage_a, stage_b, pos_ref)
        return carry

    groups = -(-ID_ROWS // 4)
    lax.fori_loop(0, groups // 2, lookup, 0)
    pl.semaphore_wait(barrier, parts - 1)
    lax.fori_loop(1, N_Z, send_z, 0)
    lax.fori_loop(groups // 2, groups, lookup, 0)
    for r in range(groups * 4, pos_ref.shape[0]):
        pos_ref[r : r + 1, :] = jnp.zeros((1, LANES), jnp.int32)
    assign(
        pos_ref, own_ref, val_ref, slot_ref, addr_ref, req_ref, parts=parts, shift=shift, cap_row=cap_row,
    )
    ask_at = pl.ds(0, 1)
    keep_req = pltpu.make_async_copy(req_ref.at[me], inbox.at[parts - 1], local_sem.at[4])
    keep_req.start()

    def ask(k, slot, other, where):
        pltpu.make_async_remote_copy(
            req_ref.at[other, ask_at], inbox.at[slot, ask_at], req_send, req_recv.at[k],
            device_id=where, device_id_type=MESH,
        ).start()

    all_peers(ask)
    hub_wait((N_Z - 1) * HOT_DEV, 0).wait_recv()
    send_x(0, x_early)
    lax.fori_loop(0, 1, send_core, 0)
    most = pl.ds(0, parts - 1)

    def asked(k, count):
        some = pl.ds(0, count)
        return pltpu.make_async_remote_copy(
            req_ref.at[some, ask_at], inbox.at[some, ask_at], req_send, req_recv.at[k],
            device_id=peer(1, 0, 1)[1], device_id_type=MESH,
        )

    def to_scalar(k):
        at = pl.ds(k * 8, 8)
        return pltpu.make_async_copy(inbox.at[at, ask_at], wanted.at[at], scalar_sem.at[k])

    asked(0, 8).wait_recv()
    to_scalar(0).start()
    keep_req.wait()

    def collect(slot):
        asked_rows = wanted.at[slot, 0]
        for i in range(cap_row):
            row_stage[i : i + 1, :] = wide[pl.ds(asked_rows[i], 1), :]
        return row_stage[...].astype(jnp.bfloat16)

    def rows_at(part):
        return pl.ds(pl.multiple_of(HUB_ROWS + part * cap_row, 8), cap_row)

    def serve(slot, dz, r):
        where = peer(dz, r, -1)[1]
        send[slot] = collect(slot)
        pltpu.make_async_remote_copy(
            send.at[slot], table_ref.at[rows_at(me)], row_send, row_recv, device_id=where, device_id_type=MESH
        ).start()
        send_x_one(slot)

    def serve_kind(k, carry):
        to_scalar(k).wait()

        @pl.when(k < N_Z - 2)
        def _():
            asked(k + 1, 8).wait_recv()
            to_scalar(k + 1).start()

        def one(r, inner):
            serve(k * 8 + r, turn_of(k), r)
            return inner

        lax.fori_loop(0, 8, one, 0)
        return carry

    lax.fori_loop(0, N_Z - 1, serve_kind, 0)
    asked(N_Z - 1, 7).wait_recv()
    to_scalar(N_Z - 1).start()
    to_scalar(N_Z - 1).wait()

    def serve_flat(r, carry):
        serve((N_Z - 1) * 8 + r - 1, 0, r)
        return carry

    lax.fori_loop(1, 8, serve_flat, 0)
    table_ref[rows_at(me), :] = collect(parts - 1)
    hub_wait((N_X - 1) * x_rows, 1).wait_recv()
    lax.fori_loop(1, N_X, send_core, 0)

    asked(0, parts - 1).wait_send()
    hub_wait((N_Z - 1) * HOT_DEV, 0).wait_send()
    hub_wait((N_X - 1) * x_rows, 1).wait_send()
    hub_wait(half, 2).wait()
    pltpu.make_async_remote_copy(
        send.at[most], send.at[most], row_send, row_recv, device_id=peer(1, 0, 1)[1], device_id_type=MESH
    ).wait()


def front(hop2, hop1, seed_ids, partition_map, features, cap_row):
    parts = lax.axis_size("dom")
    node_rows, feat = features.shape
    vmem = pl.BlockSpec(memory_space=pltpu.VMEM)
    hbm = pl.BlockSpec(memory_space=pltpu.HBM)
    rows = round_up(ID_ROWS, 8)
    table_rows = HUB_ROWS + parts * cap_row
    return pl.pallas_call(
        functools.partial(front_kernel, parts=parts, shift=node_rows.bit_length() - 1, cap_row=cap_row),
        name="front",
        out_shape=(
            jax.ShapeDtypeStruct((table_rows, feat), features.dtype),
            jax.ShapeDtypeStruct((rows, LANES), jnp.int32),
        ),
        in_specs=[hbm] * 5,
        out_specs=(vmem, vmem),
        scratch_shapes=[
            pltpu.VMEM(hop2.shape, jnp.int32),
            pltpu.VMEM(hop1.shape, jnp.int32),
            pltpu.VMEM((1, seed_ids.size), jnp.int32),
        ]
        + [pltpu.VMEM((rows, LANES), jnp.int32)] * 5
        + [
            pltpu.VMEM((partition_map.size // LANES, LANES), jnp.int32),
            pltpu.VMEM((node_rows, feat), features.dtype),
            pltpu.VMEM((node_rows, feat), jnp.float32),
            pltpu.VMEM((2 * LANES, LANES), jnp.int32),
            pltpu.VMEM((2 * LANES, LANES), jnp.int32),
            pltpu.VMEM((cap_row, feat), jnp.float32),
            pltpu.VMEM((parts, 8, LANES), jnp.int32),
            pltpu.VMEM((parts, 8, LANES), jnp.int32),
            pltpu.VMEM((parts, cap_row, feat), features.dtype),
            pltpu.SMEM((rows, LANES), jnp.int32),
            pltpu.SMEM((parts, 1, LANES), jnp.int32),
            pltpu.SemaphoreType.DMA((9,)),
            pltpu.SemaphoreType.DMA((N_Z,)),
            pltpu.SemaphoreType.DMA,
            pltpu.SemaphoreType.DMA((N_Z,)),
            pltpu.SemaphoreType.DMA((3,)),
            pltpu.SemaphoreType.DMA((3,)),
            pltpu.SemaphoreType.DMA,
            pltpu.SemaphoreType.DMA,
        ],
        compiler_params=pltpu.CompilerParams(collective_id=2, has_side_effects=True, vmem_limit_bytes=24 * MIB),
    )(
        *(
            pltpu.with_memory_space_constraint(each, pltpu.HBM)
            for each in (hop2, hop1, seed_ids.reshape(1, -1), partition_map.reshape(-1, LANES), features)
        )
    )

def fetch_kernel(addr_smem, table_ref, x_ref, table_wide, own_buf, far_buf, *, seeds, fan_one, fan_two):
    def widen(step, carry):
        at = pl.ds(pl.multiple_of(step * 128, 128), 128)
        table_wide[at, :] = table_ref[at, :].astype(jnp.float32)
        return carry

    lax.fori_loop(0, table_ref.shape[0] // 128, widen, 0)
    fetch_rows(addr_smem, table_wide, own_buf, far_buf, x_ref, seeds=seeds, fan_one=fan_one, fan_two=fan_two)


def fetch_all(addr, table, seeds, fan_one, fan_two):
    feat = table.shape[1]
    total = seeds * (1 + fan_one)
    vmem = pl.BlockSpec(memory_space=pltpu.VMEM)
    return pl.pallas_call(
        functools.partial(fetch_kernel, seeds=seeds, fan_one=fan_one, fan_two=fan_two),
        name="fetch",
        out_shape=jax.ShapeDtypeStruct((total, 2 * feat), table.dtype),
        in_specs=[pl.BlockSpec(memory_space=pltpu.SMEM), vmem],
        out_specs=vmem,
        scratch_shapes=[
            pltpu.VMEM(table.shape, jnp.float32),
            pltpu.VMEM((total, feat), jnp.float32),
            pltpu.VMEM((total, feat), jnp.float32),
        ],
        compiler_params=pltpu.CompilerParams(vmem_limit_bytes=24 * MIB),
    )(addr, table)


ROOT = 0.7978845608028654
CUBE = 0.044715


def gelu_pair(pre):
    square = pre * pre
    bend = jnp.tanh(ROOT * pre * (1.0 + CUBE * square))
    half = 0.5 * (1.0 + bend)
    slope = half + 0.5 * pre * (1.0 - bend * bend) * (ROOT * (1.0 + 3.0 * CUBE * square))
    return pre * half, slope


N_REP = 4
MEMBERS = N_X * N_REP * 2
PART_TWO = 16
PART_ONE = 24
PART = PART_TWO + PART_ONE
HIGH = 176


def early_at(block):
    return block // 2, block % 2 * 8


def late_at(block):
    return block // 3, PART_TWO + block % 3 * 8


def two_at_block(block):
    early = MEMBERS * 2
    return early_at(block) if block < early else late_at(block - early)


def put(part_ref, where, tile):
    member, to = where
    rows, lanes = tile.shape
    part_ref[member, to : to + rows, :lanes] = tile.astype(jnp.bfloat16)


def pack_two(part_ref, g_two, gb_two):
    classes, width = g_two.shape
    blocks = width // LANES * (HIGH // 8)
    for late in range(blocks - MEMBERS * 2, MEMBERS * 3):
        put(part_ref, late_at(late), jnp.zeros((8, LANES), jnp.float32))
    for h in range(width // LANES):
        cols = slice(h * LANES, (h + 1) * LANES)
        for b in range(HIGH // 8):
            tile = g_two[b * 8 : min(b * 8 + 8, classes), cols]
            if tile.shape[0] < 8:
                tile = jnp.concatenate([tile, jnp.zeros((8 - tile.shape[0], LANES), jnp.float32)], axis=0)
            put(part_ref, two_at_block(h * (HIGH // 8) + b), tile)
    member, to = two_at_block(blocks)
    put(part_ref, (member, to), gb_two[:, :LANES])
    put(part_ref, (member, to + 1), gb_two[:, LANES:])


def pack_one(part_ref, g_one, gb_one, first):
    halves = g_one.shape[1] // LANES
    each = g_one.shape[0] // 8
    member, to = two_at_block(first)
    for h in range(halves):
        cols = slice(h * LANES, (h + 1) * LANES)
        for i in range(each):
            put(part_ref, two_at_block(first + 1 + h * each + i), g_one[i * 8 : i * 8 + 8, cols])
        put(part_ref, (member, to + h), gb_one[:, cols])


def dense_kernel(
    x_ref, label_ref, self_one, neigh_one, b_one_ref, self_two, neigh_two, b_two_ref,
    loss_ref, gathered,
    slope_buf, d_buf, part_ref, box, z_two, z_one, send_sem, recv_sem, *, seeds, fan_one,
):
    hidden = self_one.shape[1]
    hops = seeds * fan_one
    me, y = lax.axis_index("dom"), lax.axis_index("rep")
    core, z, x = me & 1, (me >> 1) & (N_Z - 1), me >> 4
    mine = (x * N_REP + y) * 2 + core
    barrier = pltpu.get_barrier_semaphore()

    def near(step):
        other = mine ^ (MEMBERS - 1 - step)
        return other, {"dom": ((other >> 3) << 4) + (z << 1) + (other & 1), "rep": (other >> 1) & (N_REP - 1)}

    def far(step):
        return {"dom": (x << 4) + (((z + 4 + ((step + 1) >> 1) * (1 - 2 * (step & 1))) & (N_Z - 1)) << 1) + core, "rep": y}

    def greet_near(step, carry):
        pl.semaphore_signal(barrier, inc=1, device_id=near(step)[1], device_id_type=MESH)
        return carry

    def greet_far(step, carry):
        pl.semaphore_signal(barrier, inc=1, device_id=far(step), device_id_type=MESH)
        return carry

    lax.fori_loop(0, N_Z - 1, greet_far, 0)
    lax.fori_loop(0, MEMBERS - 1, greet_near, 0)

    w_one = jnp.concatenate([self_one[...], neigh_one[...]], axis=0)
    w_two = jnp.concatenate([self_two[...], neigh_two[...]], axis=1)
    b_one = b_one_ref[...]
    hid_sum = jnp.zeros((seeds, hidden), jnp.float32)
    act = None
    for j in range(fan_one + 1):
        at = slice(j * seeds, (j + 1) * seeds)
        act, slope = gelu_pair(dot_nn(x_ref[at, :], w_one) + b_one)
        act = act.astype(jnp.bfloat16)
        slope_buf[at, :] = slope
        if j < fan_one:
            hid_sum = hid_sum + act.astype(jnp.float32)
    hid = jnp.concatenate([act, (hid_sum * (1.0 / fan_one)).astype(jnp.bfloat16)], axis=1)
    logits = dot_nt(hid, w_two) + b_two_ref[...]
    shifted = logits - jnp.max(logits, axis=1, keepdims=True)
    log_probs = shifted - jnp.log(jnp.sum(jnp.exp(shifted), axis=1, keepdims=True))
    class_iota = lax.broadcasted_iota(jnp.int32, logits.shape, 1)
    diagonal = lax.broadcasted_iota(jnp.int32, (seeds, seeds), 0) == lax.broadcasted_iota(jnp.int32, (seeds, seeds), 1)
    label = jnp.sum(jnp.where(diagonal, label_ref[...].astype(jnp.float32), 0.0), axis=1, keepdims=True)
    target = (class_iota.astype(jnp.float32) == label).astype(jnp.float32)
    loss = jnp.sum(log_probs * target, axis=1, keepdims=True)
    loss_ref[...] = -jnp.sum(jnp.where(diagonal, loss, 0.0), axis=0, keepdims=True)
    d_logits = ((jnp.exp(log_probs) - target) * (1.0 / seeds)).astype(jnp.bfloat16)
    pack_two(part_ref, dot_tn(d_logits, hid), jnp.sum(d_logits.astype(jnp.float32), axis=0, keepdims=True))
    pl.semaphore_wait(barrier, MEMBERS + N_Z - 2)

    def copy(source, target, stage, where):
        return pltpu.make_async_remote_copy(
            source, target, send_sem.at[stage], recv_sem.at[stage], device_id=where, device_id_type=MESH
        )

    two_at, one_at = pl.ds(0, PART_TWO), pl.ds(PART_TWO, PART_ONE)

    def send_two(step, carry):
        other, where = near(step)
        copy(part_ref.at[other, two_at], box.at[mine, two_at], 0, where).start()
        return carry

    lax.fori_loop(0, MEMBERS - 1, send_two, 0)
    d_hid = dot_nn(d_logits, w_two)
    d_hop = d_hid[:, hidden:] * (1.0 / fan_one)
    for j in range(fan_one + 1):
        at = slice(j * seeds, (j + 1) * seeds)
        d_pre = ((d_hop if j < fan_one else d_hid[:, :hidden]) * slope_buf[at, :]).astype(jnp.bfloat16)
        d_buf[at, :] = d_pre
    gb_one = dot_nn(jnp.ones((8, d_buf.shape[0]), jnp.bfloat16), d_buf[...])[:1]
    pack_one(part_ref, dot_tn(x_ref[...], d_buf[...]), gb_one, 2 * hidden // LANES * (HIGH // 8) + 1)

    def send_one(step, carry):
        other, where = near(step)
        copy(part_ref.at[other, one_at], box.at[mine, one_at], 1, where).start()
        return carry

    lax.fori_loop(0, MEMBERS - 1, send_one, 0)
    box[mine] = part_ref[mine]

    def across(z_box, stage):
        def one(step, carry):
            copy(z_box.at[z], z_box.at[z], stage, far(step)).start()
            return carry

        lax.fori_loop(0, N_Z - 1, one, 0)

    def back(at, stage):
        def one(step, carry):
            copy(gathered.at[mine, at], gathered.at[mine, at], stage, near(step)[1]).start()
            return carry

        lax.fori_loop(0, MEMBERS - 1, one, 0)

    def of_near(ref, at, stage):
        some = ref.at[pl.ds(0, MEMBERS - 1), at]
        return copy(some, some, stage, near(0)[1])

    def of_far(z_box, stage):
        some = z_box.at[pl.ds(0, N_Z - 1)]
        return copy(some, some, stage, far(0))

    def total_near(first, rows):
        total = box[0, first : first + rows, :].astype(jnp.float32)
        for i in range(1, MEMBERS):
            total = total + box[i, first : first + rows, :].astype(jnp.float32)
        return total

    def total_far(z_box):
        total = z_box[0]
        for i in range(1, N_Z):
            total = total + z_box[i]
        return total.astype(jnp.bfloat16)

    of_near(box, two_at, 0).wait_recv()
    z_two[z] = total_near(0, PART_TWO)
    across(z_two, 2)
    of_near(box, one_at, 1).wait_recv()
    z_one[z] = total_near(PART_TWO, PART_ONE)
    across(z_one, 3)
    of_far(z_two, 2).wait_recv()
    gathered[mine, :PART_TWO, :] = total_far(z_two)
    back(two_at, 4)
    of_far(z_one, 3).wait_recv()
    gathered[mine, PART_TWO:, :] = total_far(z_one)
    back(one_at, 5)
    of_near(gathered, two_at, 4).wait()
    of_near(gathered, one_at, 5).wait()
    of_near(box, two_at, 0).wait_send()
    of_near(box, one_at, 1).wait_send()
    of_far(z_two, 2).wait_send()
    of_far(z_one, 3).wait_send()


def dense(x, labels, self_one, neigh_one, bias_one, self_two, neigh_two, bias_two, fan_one):
    seeds = labels.shape[0]
    hidden = self_one.shape[1]
    classes = self_two.shape[1]
    total = x.shape[0]
    vmem = pl.BlockSpec(memory_space=pltpu.VMEM)
    return pl.pallas_call(
        functools.partial(dense_kernel, seeds=seeds, fan_one=fan_one),
        name="dense",
        out_shape=(
            jax.ShapeDtypeStruct((1, seeds), jnp.float32),
            jax.ShapeDtypeStruct((MEMBERS, PART, LANES), jnp.bfloat16),
        ),
        in_specs=[vmem] * 8,
        out_specs=(vmem,) * 2,
        scratch_shapes=[
            pltpu.VMEM((total, hidden), jnp.float32),
            pltpu.VMEM((total, hidden), jnp.bfloat16),
            pltpu.VMEM((MEMBERS, PART, LANES), jnp.bfloat16),
            pltpu.VMEM((MEMBERS, PART, LANES), jnp.bfloat16),
            pltpu.VMEM((N_Z, PART_TWO, LANES), jnp.float32),
            pltpu.VMEM((N_Z, PART_ONE, LANES), jnp.float32),
            pltpu.SemaphoreType.DMA((6,)),
            pltpu.SemaphoreType.DMA((6,)),
        ],
        compiler_params=pltpu.CompilerParams(collective_id=1, has_side_effects=True, vmem_limit_bytes=16 * MIB),
    )(
        x,
        labels.reshape(1, seeds),
        self_one,
        neigh_one,
        bias_one.reshape(1, hidden),
        self_two.T,
        neigh_two.T,
        bias_two.reshape(1, classes),
    )


def unpack_kernel(gathered, loss_in, loss_out, self_one, neigh_one, bias_one, self_two, neigh_two, bias_two):
    feat, hidden = self_one.shape
    classes = self_two.shape[0]
    loss_out[...] = loss_in[...]
    halves = hidden // LANES
    each = feat // 8
    blocks = 2 * halves * (HIGH // 8)

    def tile_of(block):
        member, to = two_at_block(block)
        return gathered[member, to : to + 8, :].astype(jnp.float32)

    for h in range(halves):
        cols = slice(h * LANES, (h + 1) * LANES)
        for i in range(each):
            at = slice(i * 8, (i + 1) * 8)
            self_one[at, cols] = tile_of(blocks + 2 + h * 2 * each + i)
            neigh_one[at, cols] = tile_of(blocks + 2 + h * 2 * each + each + i)
        for b in range(HIGH // 8):
            rows = min(8, classes - b * 8)
            for k, out in enumerate((self_two, neigh_two)):
                out[b * 8 : b * 8 + rows, cols] = tile_of((k * halves + h) * (HIGH // 8) + b)[:rows]
        bias_one[:, cols] = tile_of(blocks + 1)[h : h + 1]
    last = tile_of(blocks)
    bias_two[:, :LANES] = last[:1]
    bias_two[:, LANES:] = last[1:2, : classes - LANES]


def unpack(gathered, loss, feat, hidden, classes):
    vmem = pl.BlockSpec(memory_space=pltpu.VMEM)
    shapes = [loss.shape, (feat, hidden), (feat, hidden), (1, hidden), (classes, hidden), (classes, hidden), (1, classes)]
    return pl.pallas_call(
        unpack_kernel,
        name="unpack",
        out_shape=tuple(jax.ShapeDtypeStruct(shape, jnp.float32) for shape in shapes),
        in_specs=[vmem] * 2,
        out_specs=(vmem,) * 7,
        compiler_params=pltpu.CompilerParams(vmem_limit_bytes=8 * MIB),
    )(gathered, loss)


def shards(
    features, partition_map, seed_ids, hop1_ids, hop2_ids, labels,
    self_one, neigh_one, bias_one, self_two, neigh_two, bias_two,
):
    parts = lax.axis_size("dom")
    seeds = seed_ids.shape[0]
    fan_one = hop1_ids.shape[1]
    fan_two = hop2_ids.shape[2]
    feat = features.shape[1]
    tree_rows = 1 + fan_one + fan_one * fan_two
    cold_cap = tree_rows // 2 * (seeds // parts)
    cap_row = round_up(cold_cap, 8)
    table, addr = front(hop2_ids.transpose(2, 1, 0), hop1_ids.T, seed_ids, partition_map, features, cap_row)
    x = fetch_all(addr, table, seeds, fan_one, fan_two)
    hidden, classes = self_two.shape
    loss, gathered = dense(x, labels, self_one, neigh_one, bias_one, self_two, neigh_two, bias_two, fan_one)
    loss, *grads = unpack(gathered, loss, feat, hidden, classes)
    return (
        loss.reshape(-1), grads[0], grads[1], grads[2].reshape(-1),
        grads[3].T, grads[4].T, grads[5].reshape(-1),
    )


def solution(mesh):
    return jax.shard_map(
        shards,
        mesh=mesh,
        in_specs=(
            P("dom", None),
            P(),
            P(("dom", "rep")),
            P(("dom", "rep"), None),
            P(("dom", "rep"), None, None),
            P(("dom", "rep")),
            P(),
            P(),
            P(),
            P(),
            P(),
            P(),
        ),
        out_specs=(P(("dom", "rep")), P(), P(), P(), P(), P(), P()),
        check_vma=False,
    )
```
